128 devices in a mesh: ctx: 16 (over z, x), tp: 8 (over y, core).
Axes of the slice: x: 4, y: 4, z: 4, core: 2. Of those that a mesh axis runs over, the one named last changes fastest.
Arguments:
- hidden_in: bfloat16 [8192, 5376], P(('ctx', 'tp')), may hold values from -6 to 6
- stretch_start: int32 [1], replicated, may hold values from 1 to 1024
- pre_gain: float32 [5376], replicated, may hold values from 0.1 to 1.9
- q_weight: bfloat16 [5376, 4096], P('ctx', 'tp'), may hold values from -1 to 1
- k_weight: bfloat16 [5376, 2048], P('ctx', 'tp'), may hold values from -1 to 1
- v_weight: bfloat16 [5376, 2048], P('ctx', 'tp'), may hold values from -0.078125 to 0.078125
- o_weight: bfloat16 [4096, 5376], P('tp', 'ctx'), may hold values from -0.09375 to 0.09375
- q_gain: float32 [128], replicated, may hold values from 0.5 to 5
- k_gain: float32 [128], replicated, may hold values from 0.5 to 5
- prior_keys: bfloat16 [1024, 2048], P(None, 'tp'), may hold values from -6 to 6
- prior_values: bfloat16 [1024, 2048], P(None, 'tp'), may hold values from -6 to 6
- post_gain: float32 [5376], replicated, may hold values from 0.1 to 1.9
Outputs:
- result: bfloat16 [8192, 5376], P(('ctx', 'tp'))
The draws below stay inside these ranges and needn't reach their ends.
All inputs are finite; a program needn't handle non-finite values.
Results may differ from the reference program's by a relative error of at most 0.013.
Values may be sent and summed in bfloat16 or wider, within the bound.
A program may use at most 128 MiB of HBM per device.

```python
import jax
import jax.numpy as jnp
from jax import lax

D = 5376
HEADS = 32
KVH = 16
HD = 128
WINDOW = 1024
TOK_DEV = 512
TOKENS = 8192


def query_base(key):
    normal_q = jax.random.normal(jax.random.fold_in(key, 11), (D, HEADS * HD), jnp.float32)
    return jnp.clip(normal_q, -6.0, 6.0) / jnp.sqrt(jnp.float32(D))


def draw_q_weight(key, part):
    return query_base(key).astype(jnp.bfloat16)


def draw_k_weight(key, part):
    normal_k = jax.random.normal(jax.random.fold_in(key, 12), (D, KVH * HD), jnp.float32)
    own_part = jnp.clip(normal_k, -6.0, 6.0) / jnp.sqrt(jnp.float32(D))
    return own_part.astype(jnp.bfloat16)


def gain_draw(key, salt):
    unit = jax.random.uniform(jax.random.fold_in(key, salt), (HD,), jnp.float32)
    return jnp.exp(jnp.log(0.6) + unit * (jnp.log(1.6) - jnp.log(0.6)))


def draw_q_gain(key, part):
    return gain_draw(key, 21)


def draw_k_gain(key, part):
    return gain_draw(key, 22)


def shard_levels(key, shape, shards, low, high):
    factor_of, own = 1.0, jax.random.fold_in(key, 6)
    for dim, parts in shards:
        draws = jnp.exp(jax.random.uniform(jax.random.fold_in(own, dim), (parts,), jnp.float32, low / len(shards), high / len(shards)))
        factor_of = factor_of * jnp.repeat(draws, shape[dim] // parts).reshape([-1 if axis == dim else 1 for axis in range(len(shape))])
    return factor_of


def centred(key, dims, scale, most, shards=(), held_as=jnp.bfloat16):
    array = jax.random.normal(key, dims, jnp.float32) * scale
    if len(shards) > 0:
        array = shard_levels(key, dims, shards, -0.22, 0.18) * array
    return jnp.clip(array, min=-most, max=most).astype(held_as)


def setup_inputs(seed: int = 0) -> dict:
    seeds = jax.random.split(jax.random.key(seed), 13)
    return {
        "hidden_in": centred(seeds[0], (TOKENS, D), 1.0, 6.0, ((0, 128),)),
        "stretch_start": jax.random.randint(seeds[1], (1,), 1, WINDOW + 1).astype(jnp.int32),
        "pre_gain": jnp.clip(1.0 + 0.18 * jax.random.normal(seeds[2], (D,), jnp.float32), 0.1, 1.9),
        "q_weight": draw_q_weight(jax.random.fold_in(seeds[12], 71), 0),
        "k_weight": draw_k_weight(jax.random.fold_in(seeds[12], 71), 0),
        "v_weight": centred(seeds[5], (D, KVH * HD), D ** -0.5, 0.078125, ((0, 16), (1, 8))),
        "o_weight": centred(seeds[6], (HEADS * HD, D), (HEADS * HD) ** -0.5, 0.09375, ((0, 8), (1, 16))),
        "q_gain": draw_q_gain(jax.random.fold_in(seeds[12], 71), 0),
        "k_gain": draw_k_gain(jax.random.fold_in(seeds[12], 71), 0),
        "prior_keys": centred(seeds[9], (WINDOW, KVH * HD), 1.0, 6.0, ((1, 8),)),
        "prior_values": centred(seeds[10], (WINDOW, KVH * HD), 1.0, 6.0, ((1, 8),)),
        "post_gain": jnp.clip(1.0 + 0.18 * jax.random.normal(seeds[11], (D,), jnp.float32), 0.1, 1.9),
    }


EPSILON = 1e-06
QUERY_FACTOR = 168.0 ** (-0.5)

def rms_scale(inputs, scales):
    mean_sq = lax.optimization_barrier(jnp.mean(inputs * inputs, axis=-1, keepdims=True))
    return inputs * lax.rsqrt(mean_sq + EPSILON) * scales

def rotate(inputs, positions):
    half_dim = inputs.shape[-1] // 2
    frequency = 10000.0 ** (-jnp.arange(half_dim, dtype=jnp.float32) / half_dim)
    angles = positions.astype(jnp.float32)[:, None] * frequency[None, :]
    cosines = jnp.cos(angles)[:, None, :]
    sines = jnp.sin(angles)[:, None, :]
    front = inputs[..., :half_dim]
    second = inputs[..., half_dim:]
    return jnp.concatenate([front * cosines - second * sines, second * cosines + front * sines], axis=-1)

def reference(hidden_in, stretch_start, pre_gain, q_weight, k_weight, v_weight, o_weight, q_gain, k_gain, prior_keys, prior_values, post_gain):
    residual_in = hidden_in.astype(jnp.float32)
    normed = rms_scale(residual_in, pre_gain).astype(jnp.bfloat16)
    positions = WINDOW + jnp.arange(TOKENS, dtype=jnp.int32)
    query_raw = jnp.dot(normed, q_weight, preferred_element_type=jnp.float32).reshape(TOKENS, HEADS, HD)
    query = (rotate(rms_scale(query_raw, q_gain), positions) * QUERY_FACTOR).astype(jnp.bfloat16)
    key_raw = jnp.dot(normed, k_weight, preferred_element_type=jnp.float32).reshape(TOKENS, KVH, HD)
    key_rows = rotate(rms_scale(key_raw, k_gain), positions).astype(jnp.bfloat16).reshape(TOKENS, KVH * HD)
    value_rows = jnp.dot(normed, v_weight, preferred_element_type=jnp.float32).astype(jnp.bfloat16)
    all_keys = jnp.concatenate([prior_keys, key_rows], axis=0)
    all_values = jnp.concatenate([prior_values, value_rows], axis=0)
    first_valid = WINDOW - stretch_start[0]
    group = HEADS // KVH
    span = WINDOW + TOK_DEV

    def one_block(block_index):
        offset = (block_index * TOK_DEV).astype(jnp.int32)
        query_block = lax.dynamic_slice_in_dim(query, offset, TOK_DEV, 0).astype(jnp.float32)
        key_block = lax.dynamic_slice_in_dim(all_keys, offset, span, 0).reshape(span, KVH, HD)
        value_block = lax.dynamic_slice_in_dim(all_values, offset, span, 0).reshape(span, KVH, HD)
        key_block = jnp.repeat(key_block, group, axis=1).astype(jnp.float32)
        value_block = jnp.repeat(value_block, group, axis=1).astype(jnp.float32)
        scores = jnp.einsum('qhd,khd->hqk', query_block, key_block)
        query_pos = WINDOW + offset + jnp.arange(TOK_DEV, dtype=jnp.int32)
        key_pos = offset + jnp.arange(span, dtype=jnp.int32)
        allowed = (key_pos[None, :] <= query_pos[:, None]) & (key_pos[None, :] > query_pos[:, None] - WINDOW) & (key_pos[None, :] >= first_valid)
        scores = jnp.where(allowed[None, :, :], scores, jnp.float32(-1e+30))
        largest = lax.optimization_barrier(jnp.max(scores, axis=-1, keepdims=True))
        expon = jnp.exp(scores - largest)
        attn_probs = (expon / lax.optimization_barrier(jnp.sum(expon, axis=-1, keepdims=True))).astype(jnp.bfloat16)
        attended = jnp.einsum('hqk,khd->qhd', attn_probs.astype(jnp.float32), value_block)
        return attended.astype(jnp.bfloat16).reshape(TOK_DEV, HEADS * HD)
    blocks = lax.map(one_block, jnp.arange(TOKENS // TOK_DEV, dtype=jnp.int32))
    attended = blocks.reshape(TOKENS, HEADS * HD)
    projected = jnp.dot(attended, o_weight, preferred_element_type=jnp.float32)
    return (residual_in + rms_scale(projected, post_gain)).astype(jnp.bfloat16)
```

```python
import jax
import jax.numpy as jnp
from jax import lax
from jax.experimental import pallas as pl
from jax.experimental.pallas import tpu as pltpu
from jax.sharding import PartitionSpec as P

HD = 128
WINDOW = 1024
EPSILON = 1e-06
QUERY_FACTOR = 168.0 ** (-0.5)
MESH = pl.DeviceIdType.MESH

D = 5376
BLK = 336
NC = 512
TOK = 512
SUB = 64
CH = 1344
CHP = 1408
SPLIT = ((0, 192, 96), (192, 144, 80))
KT = 768
BF = jnp.bfloat16
F32 = jnp.float32


def body(
    hid_h, start_s, pre_v, q_h, k_h, v_h, o_h, qg_v, kg_v, pk_h, pv_h, post_v, cos_v, sin_v,
    out_v,
    w0, w1, w2, xs, kv, qb, att, acc, hid, pp, dd, ee, gg, cb, ss,
    lsem, wsend, wrecv, xsend, xrecv, kvsend, kvrecv, rsend, rrecv,
):
    c = lax.axis_index("ctx")
    t = lax.axis_index("tp")
    z, x = c // 4, c % 4
    y, core = t // 2, t % 2
    ws = (w0, w1, w2)

    def nxt(a, d):
        return (a + d + 4) % 4

    yp, ym, yo = nxt(y, 1), nxt(y, -1), nxt(y, 2)
    other = 1 - core
    to_yp = {"ctx": c, "tp": yp * 2 + core}
    to_ym = {"ctx": c, "tp": ym * 2 + core}
    to_pt = {"ctx": c, "tp": y * 2 + other}

    def dev(ci):
        return {"ctx": ci, "tp": t}

    own = pl.ds(pl.multiple_of(c * BLK, 16), BLK)
    loads = [
        pltpu.make_async_copy(k_h, w0.at[own, pl.ds(0, 256)], lsem.at[0]),
        pltpu.make_async_copy(v_h, w0.at[own, pl.ds(256, 256)], lsem.at[1]),
        pltpu.make_async_copy(hid_h, hid, lsem.at[2]),
        pltpu.make_async_copy(q_h, w1.at[own, :], lsem.at[3]),
        pltpu.make_async_copy(o_h, w2.at[own, :], lsem.at[4]),
    ]
    for load in loads:
        load.start()

    def prior(g, half, sem):
        rows = pl.ds(half * 512, 512)
        src = (pk_h, pv_h)[g // 2]
        return pltpu.make_async_copy(
            src.at[rows, pl.ds((g % 2) * HD, HD)], kv.at[g, rows, :], lsem.at[sem]
        )

    @pl.when(c == 0)
    def _():
        for g in range(4):
            prior(g, 0, 5 + g).start()
            prior(g, 1, 9 + g).start()

    @pl.when(c == 1)
    def _():
        for g in range(4):
            pltpu.make_async_copy(
                (pk_h, pv_h)[g // 2].at[pl.ds(512, 512), pl.ds((g % 2) * HD, HD)],
                kv.at[g, pl.ds(0, 512), :],
                lsem.at[5 + g],
            ).start()

    barrier = pltpu.get_barrier_semaphore()
    peers = [to_yp, to_ym, to_pt]
    peers += [dev(z * 4 + nxt(x, 1)), dev(z * 4 + nxt(x, -1))]
    peers += [dev(nxt(z, 1) * 4 + x), dev(nxt(z, -1) * 4 + x)]
    peers += [dev((c + 1) % 16), dev((c + 15) % 16)]
    for peer in peers:
        pl.semaphore_signal(barrier, inc=1, device_id=peer, device_id_type=MESH)
    pl.semaphore_wait(barrier, len(peers))

    def fs(col):
        return (x, z) if col == 0 else (z, x)

    def cid(col, f, s):
        return s * 4 + f if col == 0 else f * 4 + s

    def rows_of(col, f, s, part):
        r0, n, h = SPLIT[col]
        off, num = ((r0, n), (r0, h), (r0 + h, n - h))[part]
        return pl.ds(pl.multiple_of(cid(col, f, s) * BLK + off, 16), num)

    def wcopy(p, col, f, s, part, sem, df, ds):
        f0, s0 = fs(col)
        ref = ws[p].at[rows_of(col, f, s, part), :]
        return pltpu.make_async_remote_copy(
            src_ref=ref, dst_ref=ref, send_sem=wsend.at[p], recv_sem=wrecv.at[p, col * 20 + sem],
            device_id=dev(cid(col, nxt(f0, df), nxt(s0, ds))), device_id_type=MESH,
        )

    def got(p, col, f, s, part, sem):
        wcopy(p, col, f, s, part, sem, 1, 0).wait_recv()

    JF = (0, -1, 1, 2)

    def i0(p):
        for col in range(2):
            f, s = fs(col)
            wcopy(p, col, f, s, 0, 0, 1, 0).start()
            wcopy(p, col, f, s, 0, 1, -1, 0).start()
        for col in range(2):
            f, s = fs(col)
            wcopy(p, col, f, s, 0, 4, 0, 1).start()
            wcopy(p, col, f, s, 0, 5, 0, -1).start()

    def s1(p):
        for col in range(2):
            f, s = fs(col)
            got(p, col, nxt(f, -1), s, 0, 0)
            wcopy(p, col, nxt(f, -1), s, 1, 2, 1, 0).start()
            got(p, col, nxt(f, 1), s, 0, 1)
            wcopy(p, col, nxt(f, 1), s, 2, 3, -1, 0).start()
        for col in range(2):
            f, s = fs(col)
            for j in (1, 2):
                fj = nxt(f, JF[j])
                wcopy(p, col, fj, s, 0, 4 + 2 * j, 0, 1).start()
                wcopy(p, col, fj, s, 0, 5 + 2 * j, 0, -1).start()

    def fwd(p, j):
        for col in range(2):
            f, s = fs(col)
            fj = nxt(f, JF[j])
            got(p, col, fj, nxt(s, -1), 0, 4 + 2 * j)
            wcopy(p, col, fj, nxt(s, -1), 1, 12 + 2 * j, 0, 1).start()
            got(p, col, fj, nxt(s, 1), 0, 5 + 2 * j)
            wcopy(p, col, fj, nxt(s, 1), 2, 13 + 2 * j, 0, -1).start()

    def s3(p):
        for col in range(2):
            f, s = fs(col)
            fo = nxt(f, 2)
            got(p, col, fo, s, 1, 2)
            got(p, col, fo, s, 2, 3)
            wcopy(p, col, fo, s, 0, 10, 0, 1).start()
            wcopy(p, col, fo, s, 0, 11, 0, -1).start()

    def last(p, col, j):
        f, s = fs(col)
        fj = nxt(f, JF[j])
        got(p, col, fj, nxt(s, 2), 1, 12 + 2 * j)
        got(p, col, fj, nxt(s, 2), 2, 13 + 2 * j)

    def s6(p):
        for j in range(4):
            for col in range(2):
                last(p, col, j)

    def drain(p):
        ref = ws[p].at[pl.ds(0, 15 * BLK), :]
        pltpu.make_async_remote_copy(
            src_ref=ref, dst_ref=ref, send_sem=wsend.at[p], recv_sem=wrecv.at[p, 0],
            device_id=to_pt, device_id_type=MESH,
        ).wait_send()

    def xcopy(yy, kk, part, sem, to):
        off, num = ((0, SUB), (0, SUB // 2), (SUB // 2, SUB // 2))[part]
        ref = xs.at[pl.ds(pl.multiple_of((yy * 2 + kk) * SUB + off, 16), num), :]
        return pltpu.make_async_remote_copy(
            src_ref=ref, dst_ref=ref, send_sem=xsend, recv_sem=xrecv.at[sem],
            device_id=to, device_id_type=MESH,
        )

    loads[0].wait()
    loads[1].wait()
    i0(0)

    loads[2].wait()

    def prenorm(i, carry):
        rows = pl.ds(pl.multiple_of(i * 16, 16), 16)
        h = hid[rows, :].astype(F32)
        r = lax.rsqrt(jnp.mean(h * h, axis=-1, keepdims=True) + EPSILON)
        xs[pl.ds(pl.multiple_of(t * SUB + i * 16, 16), 16), :] = (h * r * pre_v[...]).astype(BF)
        return carry

    lax.fori_loop(0, SUB // 16, prenorm, 0)
    xcopy(y, core, 0, 0, to_yp).start()
    xcopy(y, core, 0, 1, to_ym).start()
    xcopy(y, core, 0, 4, to_pt).start()

    s1(0)
    fwd(0, 0)
    s3(0)
    fwd(0, 1)
    fwd(0, 2)
    xcopy(ym, core, 0, 0, to_yp).wait_recv()
    xcopy(ym, core, 1, 2, to_yp).start()
    xcopy(ym, core, 0, 5, to_pt).start()
    xcopy(yp, core, 0, 1, to_ym).wait_recv()
    xcopy(yp, core, 2, 3, to_ym).start()
    xcopy(yp, core, 0, 6, to_pt).start()
    loads[3].wait()
    fwd(0, 3)
    i0(1)
    xcopy(yo, core, 1, 2, to_yp).wait_recv()
    xcopy(yo, core, 2, 3, to_yp).wait_recv()
    xcopy(yo, core, 0, 7, to_pt).start()
    s6(0)
    xcopy(y, other, 0, 4, to_pt).wait_recv()
    xcopy(ym, other, 0, 5, to_pt).wait_recv()
    xcopy(yp, other, 0, 6, to_pt).wait_recv()
    xcopy(yo, other, 0, 7, to_pt).wait_recv()

    def mm(w, c0, cols):
        def step(i, carry):
            ks = pl.ds(pl.multiple_of(i * KT, 128), KT)
            acc[:, c0:c0 + cols] += jnp.dot(
                xs[:, ks], w[ks, c0:c0 + cols], preferred_element_type=F32
            )
            return carry

        acc[:, c0:c0 + cols] = jnp.zeros((TOK, cols), F32)
        lax.fori_loop(0, D // KT, step, 0)

    def headed(c0, gain):
        raw = acc[:, c0:c0 + HD]
        r = lax.rsqrt(jnp.mean(raw * raw, axis=-1, keepdims=True) + EPSILON)
        n = raw * r * gain[...]
        return n * cos_v[...] + pltpu.roll(n, HD // 2, 1) * sin_v[...]

    own_rows = pl.ds(WINDOW, TOK)
    mm(w0, 0, 256)
    s1(1)
    mm(w0, 256, 256)
    for g in range(2):
        kv[g, own_rows, :] = headed(g * HD, kg_v).astype(BF)
        kv[2 + g, own_rows, :] = acc[:, 256 + g * HD:256 + (g + 1) * HD].astype(BF)

    def kvcopy(src, dst, sem):
        return pltpu.make_async_remote_copy(
            src_ref=kv.at[:, pl.ds(src, TOK), :], dst_ref=kv.at[:, pl.ds(dst, TOK), :],
            send_sem=kvsend.at[sem], recv_sem=kvrecv.at[sem],
            device_id=dev((c + 1) % 16), device_id_type=MESH,
        )

    @pl.when(c < 15)
    def _():
        kvcopy(1024, 512, 0).start()

    fwd(1, 0)
    s3(1)
    fwd(1, 1)
    fwd(1, 2)

    @pl.when(c >= 1)
    def _():
        kvcopy(512, 512, 0).wait_recv()

    @pl.when((c >= 1) & (c < 15))
    def _():
        kvcopy(512, 0, 1).start()

    loads[4].wait()
    fwd(1, 3)
    i0(2)
    s6(1)

    mm(w1, 0, 256)
    s1(2)
    mm(w1, 256, 256)
    for h in range(4):
        qb[h, :, :] = (headed(h * HD, qg_v) * QUERY_FACTOR).astype(BF)

    @pl.when(c == 0)
    def _():
        for g in range(4):
            prior(g, 0, 5 + g).wait()
            prior(g, 1, 9 + g).wait()

    @pl.when(c == 1)
    def _():
        for g in range(4):
            pltpu.make_async_copy(
                (pk_h, pv_h)[g // 2].at[pl.ds(512, 512), pl.ds((g % 2) * HD, HD)],
                kv.at[g, pl.ds(0, 512), :],
                lsem.at[5 + g],
            ).wait()

    fwd(2, 0)

    @pl.when(c >= 2)
    def _():
        kvcopy(512, 0, 1).wait_recv()

    first = WINDOW - start_s[0] - c * TOK

    def unit(u, carry):
        g, qc = u // 4, u % 4
        q0 = pl.multiple_of(qc * 128, 128)
        q = qb[pl.ds(2 * g, 2), pl.ds(q0, 128), :].reshape(256, HD)
        k = kv[g, pl.ds(q0, 1152), :]
        v = kv[2 + g, pl.ds(q0, 1152), :]
        s = lax.dot_general(q, k, (((1,), (1,)), ((), ())), preferred_element_type=F32)
        j = lax.broadcasted_iota(jnp.int32, (256, 1152), 1)
        r = lax.broadcasted_iota(jnp.int32, (256, 1152), 0)
        r = jnp.where(r >= 128, r - 128, r)
        s = jnp.where((j > r) & (j <= r + WINDOW) & (j >= first - q0), s, F32(-1e30))
        m = jnp.max(s, axis=-1, keepdims=True)
        e = jnp.exp(s - m)
        total = jnp.sum(e, axis=-1, keepdims=True)
        o = jnp.dot(e.astype(BF), v, preferred_element_type=F32) / total
        c0 = pl.multiple_of(g * 256, 128)
        att[pl.ds(q0, 128), pl.ds(c0, 128)] = o[:128].astype(BF)
        c1 = pl.multiple_of(g * 256 + 128, 128)
        att[pl.ds(q0, 128), pl.ds(c1, 128)] = o[128:].astype(BF)
        return carry

    lax.fori_loop(0, 2, unit, 0)
    s3(2)
    lax.fori_loop(2, 4, unit, 0)
    fwd(2, 1)
    lax.fori_loop(4, 6, unit, 0)
    fwd(2, 2)
    lax.fori_loop(6, 8, unit, 0)

    zk = (z, nxt(z, -1), nxt(z, 1), nxt(z, 2))

    def rcopy(src, dst, q, sem, to):
        return pltpu.make_async_remote_copy(
            src_ref=src, dst_ref=dst, send_sem=rsend.at[q, sem], recv_sem=rrecv.at[q, sem],
            device_id=to, device_id_type=MESH,
        )

    def r0copy(q):
        return rcopy(pp.at[q, :, other], dd.at[q], q, 0, to_pt)

    def r1copy(q, half):
        return rcopy(
            cb.at[q, 0, pl.ds(half * 32, 32)], ee.at[q, half], q, 1 + half, (to_yp, to_ym)[half]
        )

    def r2copy(q, half):
        return rcopy(cb.at[q, 1 + half], gg.at[q, half], q, 3 + half, (to_yp, to_ym)[half])

    def proj(q):
        rows = pl.ds(pl.multiple_of(zk[q] * CH, 16), CH)

        def part(i, carry):
            a = att[pl.ds(pl.multiple_of(i * 256, 256), 256), :]
            o = lax.dot_general(
                a, w2[rows, :], (((1,), (1,)), ((), ())), preferred_element_type=F32
            ).astype(BF)
            for b in range(4):
                pp[q, i * 2 + b // 2, b % 2, :, 0:CH] = o[b * SUB:(b + 1) * SUB]
            return carry

        lax.fori_loop(0, 2, part, 0)
        r0copy(q).start()

    def both(q, yy):
        return pp[q, yy, core].astype(F32) + dd[q, yy].astype(F32)

    def r1(q):
        r0copy(q).wait_recv()
        cb[q, 0] = both(q, yo).astype(BF)
        r1copy(q, 0).start()
        r1copy(q, 1).start()

    def r2(q):
        r1copy(q, 0).wait_recv()
        a = both(q, yp)
        cb[q, 1, 0:32] = (a[0:32] + ee[q, 0].astype(F32)).astype(BF)
        cb[q, 1, 32:64] = a[32:64].astype(BF)
        r2copy(q, 0).start()
        r1copy(q, 1).wait_recv()
        a = both(q, ym)
        cb[q, 2, 0:32] = a[0:32].astype(BF)
        cb[q, 2, 32:64] = (a[32:64] + ee[q, 1].astype(F32)).astype(BF)
        r2copy(q, 1).start()

    def r3(q):
        r2copy(q, 0).wait_recv()
        r2copy(q, 1).wait_recv()
        ss[zk[q]] = both(q, y) + gg[q, 0].astype(F32) + gg[q, 1].astype(F32)

    for q in range(4):
        for b in range(8):
            pp[q, b // 2, b % 2, :, 1280:CHP] = jnp.zeros((SUB, CHP - 1280), BF)

    last(2, 1, 0)
    proj(0)
    fwd(2, 3)
    last(2, 1, 1)
    proj(1)
    r1(0)
    last(2, 1, 2)
    proj(2)
    r1(1)
    r2(0)
    last(2, 1, 3)
    for j in range(4):
        last(2, 0, j)
    proj(3)
    r1(2)
    r2(1)
    r1(3)
    r2(2)
    r3(0)
    r2(3)
    r3(1)
    r3(2)
    r3(3)

    lane = lax.broadcasted_iota(jnp.int32, (16, 128), 1)

    def final(i, carry):
        rows = pl.ds(pl.multiple_of(i * 16, 16), 16)
        pieces = []
        for pair in range(2):
            a = ss[2 * pair, rows, :]
            b = pltpu.roll(ss[2 * pair + 1, rows, :], 64, 1)
            mid = jnp.where(lane < 64, a[:, 1280:], b[:, :128])
            pieces += [a[:, :1280], mid, b[:, 128:]]
        v = jnp.concatenate(pieces, axis=1)
        r = lax.rsqrt(jnp.mean(v * v, axis=-1, keepdims=True) + EPSILON)
        out_v[rows, :] = (hid[rows, :].astype(F32) + v * r * post_v[...]).astype(BF)
        return carry

    lax.fori_loop(0, SUB // 16, final, 0)

    for p in range(3):
        drain(p)
    ref = xs.at[pl.ds(0, 7 * SUB), :]
    pltpu.make_async_remote_copy(
        src_ref=ref, dst_ref=ref, send_sem=xsend, recv_sem=xrecv.at[0],
        device_id=to_pt, device_id_type=MESH,
    ).wait_send()

    @pl.when(c < 15)
    def _():
        kvcopy(1024, 512, 0).wait_send()

    @pl.when((c >= 1) & (c < 15))
    def _():
        kvcopy(512, 0, 1).wait_send()

    for q in range(4):
        r0copy(q).wait_send()
        for half in range(2):
            r1copy(q, half).wait_send()
            r2copy(q, half).wait_send()


def local(
    hidden_in, stretch_start, pre_gain, q_weight, k_weight, v_weight, o_weight, q_gain, k_gain,
    prior_keys, prior_values, post_gain,
):
    c = lax.axis_index("ctx")
    positions = (WINDOW + c * TOK + jnp.arange(TOK, dtype=jnp.int32)).astype(F32)
    frequency = 10000.0 ** (-jnp.arange(HD // 2, dtype=F32) / (HD // 2))
    angles = positions[:, None] * frequency[None, :]
    cosines, sines = jnp.cos(angles), jnp.sin(angles)
    cos2 = jnp.concatenate([cosines, cosines], axis=1)
    sin2 = jnp.concatenate([-sines, sines], axis=1)
    hbm = pl.BlockSpec(memory_space=pl.ANY)
    vm = pl.BlockSpec(memory_space=pltpu.VMEM)
    sm = pl.BlockSpec(memory_space=pltpu.SMEM)
    dma = pltpu.SemaphoreType.DMA
    return pl.pallas_call(
        body,
        out_shape=jax.ShapeDtypeStruct((SUB, D), BF),
        in_specs=[hbm, sm, vm, hbm, hbm, hbm, hbm, vm, vm, hbm, hbm, vm, vm, vm],
        out_specs=vm,
        scratch_shapes=[
            pltpu.VMEM((D, NC), BF), pltpu.VMEM((D, NC), BF), pltpu.VMEM((D, NC), BF),
            pltpu.VMEM((TOK, D), BF),
            pltpu.VMEM((4, WINDOW + TOK, HD), BF),
            pltpu.VMEM((4, TOK, HD), BF),
            pltpu.VMEM((TOK, NC), BF),
            pltpu.VMEM((TOK, NC), F32),
            pltpu.VMEM((SUB, D), BF),
            pltpu.VMEM((4, 4, 2, SUB, CHP), BF),
            pltpu.VMEM((4, 4, SUB, CHP), BF),
            pltpu.VMEM((4, 2, SUB // 2, CHP), BF),
            pltpu.VMEM((4, 2, SUB, CHP), BF),
            pltpu.VMEM((4, 3, SUB, CHP), BF),
            pltpu.VMEM((4, SUB, CHP), F32),
            dma((16,)), dma((3,)), dma((3, 40)), dma, dma((8,)), dma((2,)), dma((2,)),
            dma((4, 5)), dma((4, 5)),
        ],
        compiler_params=pltpu.CompilerParams(
            collective_id=0, has_side_effects=True, vmem_limit_bytes=64 * 1024 * 1024 - 128 * 1024
        ),
        name="layer",
    )(
        hidden_in, stretch_start, pre_gain.reshape(1, D), q_weight, k_weight, v_weight,
        o_weight.T, q_gain.reshape(1, HD), k_gain.reshape(1, HD), prior_keys, prior_values,
        post_gain.reshape(1, D), cos2, sin2,
    )


def solution(mesh):
    return jax.shard_map(
        local,
        mesh=mesh,
        in_specs=(
            P(("ctx", "tp"), None), P(), P(), P("ctx", "tp"), P("ctx", "tp"), P("ctx", "tp"),
            P("tp", "ctx"), P(), P(), P(None, "tp"), P(None, "tp"), P(),
        ),
        out_specs=P(("ctx", "tp"), None),
        check_vma=False,
    )
```

```python
import jax
import jax.numpy as jnp
from jax import lax
from jax.experimental import pallas as pl
from jax.experimental.pallas import tpu as pltpu
from jax.sharding import PartitionSpec as P

HD = 128
WINDOW = 1024
EPSILON = 1e-06
QUERY_FACTOR = 168.0 ** (-0.5)
MESH = pl.DeviceIdType.MESH

D = 5376
BLK = 336
TOK = 512
PAIR = 1024
SUB = 64
HALF = (0, 336), (0, 176), (176, 160)
ON = (144, 192)
OH = ((0, 144), (0, 80), (80, 64)), ((0, 192), (0, 96), (96, 96))
CW = (576, 768)
CWP = (640, 768)
KT = 768
BF = jnp.bfloat16
F32 = jnp.float32
FL = set()


def body(
    hid_h, start_s, pre_h, q_h, k_h, v_h, o_h, qg_v, kg_v, pk_h, pv_h, post_h, freq_v,
    out_v,
    w0, w1, oa, ob, ow, rb, xs, kv, kr, qb, att, ast, acc, hid, pre, post, cos, sin,
    pp, dd, ee, gg, cb, sa, sb, full,
    lsem, wsend, wrecv, osend, orecv, xsend, xrecv, krsend, krrecv, kfsend, kfrecv,
    swsend, swrecv, rsend, rrecv,
):
    c = lax.axis_index("ctx")
    t = lax.axis_index("tp")
    z, x = c // 4, c % 4
    y, core = t // 2, t % 2
    b = x % 2
    nb = 1 - b
    ws = (w0, w1)

    def nxt(a, d):
        return (a + d + 4) % 4

    def pairx(xx):
        return xx + 1 - 2 * (xx % 2)

    def otherx(xx):
        return (xx + 3 + 2 * (xx % 2)) % 4

    xq, xn, xo = pairx(x), otherx(x), nxt(x, 2)
    yp, ym, yo = nxt(y, 1), nxt(y, -1), nxt(y, 2)
    other = 1 - core
    to_yp = {"ctx": c, "tp": yp * 2 + core}
    to_ym = {"ctx": c, "tp": ym * 2 + core}
    to_pt = {"ctx": c, "tp": y * 2 + other}

    def dev(ci):
        return {"ctx": ci, "tp": t}

    to_xq, to_xn = dev(z * 4 + xq), dev(z * 4 + xn)
    to_zp, to_zm = dev(nxt(z, 1) * 4 + x), dev(nxt(z, -1) * 4 + x)

    def remote(src, dst, ssem, rsem, to):
        return pltpu.make_async_remote_copy(
            src_ref=src, dst_ref=dst, send_sem=ssem, recv_sem=rsem, device_id=to,
            device_id_type=MESH,
        )

    own = pl.ds(pl.multiple_of(c * BLK, 16), BLK)
    hc = pl.ds(pl.multiple_of(b * HD, HD), HD)
    lo, hi = pl.ds(0, HD), pl.ds(HD, HD)
    loads0 = [
        pltpu.make_async_copy(k_h.at[:, lo], ow.at[0, 0, :, lo], lsem.at[0]),
        pltpu.make_async_copy(v_h.at[:, lo], ow.at[0, 0, :, hi], lsem.at[1]),
        pltpu.make_async_copy(k_h.at[:, hi], ow.at[0, 1, :, lo], lsem.at[2]),
        pltpu.make_async_copy(v_h.at[:, hi], ow.at[0, 1, :, hi], lsem.at[3]),
        pltpu.make_async_copy(k_h.at[:, hc], w0.at[own, lo], lsem.at[4]),
        pltpu.make_async_copy(v_h.at[:, hc], w0.at[own, hi], lsem.at[5]),
    ]
    loadx = [
        pltpu.make_async_copy(hid_h, hid, lsem.at[6]),
        pltpu.make_async_copy(pre_h, pre.at[0], lsem.at[7]),
    ]
    loads1 = [
        pltpu.make_async_copy(q_h.at[:, pl.ds(0, 256)], ow.at[1, 0], lsem.at[8]),
        pltpu.make_async_copy(q_h.at[:, pl.ds(256, 256)], ow.at[1, 1], lsem.at[9]),
        pltpu.make_async_copy(
            q_h.at[:, pl.ds(pl.multiple_of(b * 256, 256), 256)], w1.at[own, :], lsem.at[10]
        ),
    ]
    loads2 = [
        pltpu.make_async_copy(
            o_h.at[pl.ds(0, ON[0]), :],
            oa.at[pl.ds(pl.multiple_of(c * ON[0], 16), ON[0]), :], lsem.at[11],
        ),
        pltpu.make_async_copy(
            o_h.at[pl.ds(ON[0], ON[1]), :],
            ob.at[pl.ds(pl.multiple_of((x * 4 + z) * ON[1], 16), ON[1]), :], lsem.at[12],
        ),
        pltpu.make_async_copy(post_h, post.at[0], lsem.at[13]),
    ]
    for load in loads0 + loadx + loads1 + loads2:
        load.start()

    def prior(i):
        return pltpu.make_async_copy(
            (pk_h, pv_h)[i].at[:, hc], kv.at[i, pl.ds(0, WINDOW), :], lsem.at[14 + i]
        )

    @pl.when(c < 2)
    def _():
        prior(0).start()
        prior(1).start()

    cq, cn = z * 4 + xq, z * 4 + xn
    behind = (c + 14) % 16
    zb, xb = behind // 4, behind % 4
    barrier = pltpu.get_barrier_semaphore()
    peers = [to_yp, to_ym, to_pt, to_xq, to_xn, to_zp, to_zm]
    peers += [dev((cq + 2) % 16), dev((cn + 2) % 16)]
    peers += [dev(zb * 4 + pairx(xb)), dev(zb * 4 + otherx(xb))]
    for peer in peers:
        pl.semaphore_signal(barrier, inc=1, device_id=peer, device_id_type=MESH)
    pl.semaphore_wait(barrier, len(peers))

    XJ = (x, xq, xn, xo)

    def wrows(zz, xx, part):
        off, num = HALF[part]
        return pl.ds(pl.multiple_of((zz * 4 + xx) * BLK + off, 16), num)

    def wx(p, src, xx, part, sem, to):
        return remote(
            src, ws[p].at[wrows(z, xx, part), :], wsend.at[p], wrecv.at[p, sem], to
        )

    def wz(p, zz, j, part, sem, to):
        ref = ws[p].at[wrows(zz, XJ[j], part), :]
        return remote(ref, ref, wsend.at[p], wrecv.at[p, sem], to)

    def relay_in(p, side, to):
        off, num = HALF[1 + side]
        return remote(
            ow.at[p, b, pl.ds(off, num), :], rb.at[p, side, pl.ds(0, num), :],
            wsend.at[p], wrecv.at[p, 2 + side], to,
        )

    def wx0(p):
        relay_in(p, 0, to_xq).start()
        relay_in(p, 1, to_xn).start()
        wx(p, ow.at[p, nb], x, 0, 0, to_xq).start()
        wx(p, ow.at[p, nb], x, 0, 1, to_xn).start()

    def wz0(p, j):
        wz(p, z, j, 0, 6 + 2 * j, to_zp).start()
        wz(p, z, j, 0, 7 + 2 * j, to_zm).start()

    def wx1(p):
        relay_in(p, 0, to_xq).wait_recv()
        wx(p, rb.at[p, 0, pl.ds(0, HALF[1][1]), :], xq, 1, 4, to_xn).start()
        relay_in(p, 1, to_xn).wait_recv()
        wx(p, rb.at[p, 1, pl.ds(0, HALF[2][1]), :], xn, 2, 5, to_xq).start()

    def wz1(p):
        wx(p, ow.at[p, nb], xq, 0, 0, to_xq).wait_recv()
        wz0(p, 1)
        wx(p, ow.at[p, nb], xn, 0, 1, to_xn).wait_recv()
        wz0(p, 2)

    def wz2(p):
        wx(p, rb.at[p, 0, pl.ds(0, HALF[1][1]), :], xo, 1, 4, to_xn).wait_recv()
        wx(p, rb.at[p, 1, pl.ds(0, HALF[2][1]), :], xo, 2, 5, to_xq).wait_recv()
        wz0(p, 3)

    def wfwd(p, j):
        wz(p, nxt(z, -1), j, 0, 6 + 2 * j, to_zp).wait_recv()
        wz(p, nxt(z, -1), j, 1, 14 + 2 * j, to_zp).start()
        wz(p, nxt(z, 1), j, 0, 7 + 2 * j, to_zm).wait_recv()
        wz(p, nxt(z, 1), j, 2, 15 + 2 * j, to_zm).start()

    def wlast(p):
        for j in range(4):
            wz(p, nxt(z, 2), j, 1, 14 + 2 * j, to_zp).wait_recv()
            wz(p, nxt(z, 2), j, 2, 15 + 2 * j, to_zm).wait_recv()

    JF = (0, -1, 1, 2)

    def fs(col):
        return (x, z) if col == 0 else (z, x)

    def ctx_of(col, f, s):
        return s * 4 + f if col == 0 else f * 4 + s

    def ocopy(col, f, s, part, sem, df, ds):
        f0, s0 = fs(col)
        off, num = OH[col][part]
        ref = (oa, ob)[col].at[pl.ds(pl.multiple_of((s * 4 + f) * ON[col] + off, 16), num), :]
        to = dev(ctx_of(col, nxt(f0, df), nxt(s0, ds)))
        return remote(ref, ref, osend.at[col], orecv.at[col, sem], to)

    def ogot(col, f, s, part, sem):
        ocopy(col, f, s, part, sem, 1, 0).wait_recv()

    def o0(col):
        f, s = fs(col)
        ocopy(col, f, s, 0, 0, 1, 0).start()
        ocopy(col, f, s, 0, 1, -1, 0).start()

    def o0s(col):
        f, s = fs(col)
        ocopy(col, f, s, 0, 4, 0, 1).start()
        ocopy(col, f, s, 0, 5, 0, -1).start()

    def o1(col):
        f, s = fs(col)
        ogot(col, nxt(f, -1), s, 0, 0)
        ocopy(col, nxt(f, -1), s, 1, 2, 1, 0).start()
        ogot(col, nxt(f, 1), s, 0, 1)
        ocopy(col, nxt(f, 1), s, 2, 3, -1, 0).start()

    def o1s(col):
        f, s = fs(col)
        for j in (1, 2):
            fj = nxt(f, JF[j])
            ocopy(col, fj, s, 0, 4 + 2 * j, 0, 1).start()
            ocopy(col, fj, s, 0, 5 + 2 * j, 0, -1).start()

    def o3(col):
        f, s = fs(col)
        fo = nxt(f, 2)
        ogot(col, fo, s, 1, 2)
        ogot(col, fo, s, 2, 3)
        ocopy(col, fo, s, 0, 10, 0, 1).start()
        ocopy(col, fo, s, 0, 11, 0, -1).start()

    def ofwd(col, j):
        f, s = fs(col)
        fj = nxt(f, JF[j])
        ogot(col, fj, nxt(s, -1), 0, 4 + 2 * j)
        ocopy(col, fj, nxt(s, -1), 1, 12 + 2 * j, 0, 1).start()
        ogot(col, fj, nxt(s, 1), 0, 5 + 2 * j)
        ocopy(col, fj, nxt(s, 1), 2, 13 + 2 * j, 0, -1).start()

    def olast(col):
        f, s = fs(col)
        for j in range(4):
            fj = nxt(f, JF[j])
            ogot(col, fj, nxt(s, 2), 1, 12 + 2 * j)
            ogot(col, fj, nxt(s, 2), 2, 13 + 2 * j)

    def xcopy(cc, yy, kk, part, sem, to):
        off, num = ((0, SUB), (0, SUB // 2), (SUB // 2, SUB // 2))[part]
        ref = xs.at[pl.ds(pl.multiple_of(cc * TOK + (yy * 2 + kk) * SUB + off, 16), num), :]
        return remote(ref, ref, xsend, xrecv.at[sem], to)

    def xhop(cc, s):
        xcopy(cc, ym, core, 0, 1 + s, to_yp).wait_recv()
        xcopy(cc, ym, core, 1, 4 + s, to_yp).start()
        xcopy(cc, yp, core, 0, 2 + s, to_ym).wait_recv()
        xcopy(cc, yp, core, 2, 5 + s, to_ym).start()
        xcopy(cc, ym, core, 0, 13 + s // 2, to_pt).start()
        xcopy(cc, yp, core, 0, 14 + s // 2, to_pt).start()

    def xopp(cc, s):
        xcopy(cc, yo, core, 1, 4 + s, to_yp).wait_recv()
        xcopy(cc, yo, core, 2, 5 + s, to_ym).wait_recv()
        xcopy(cc, yo, core, 0, 15 + s // 2, to_pt).start()

    def xsend0(cc, s):
        xcopy(cc, y, core, 0, 1 + s, to_yp).start()
        xcopy(cc, y, core, 0, 2 + s, to_ym).start()
        xcopy(cc, y, core, 0, 3 + s, to_pt).start()

    def xdone(cc, s):
        xcopy(cc, y, other, 0, 3 + s, to_pt).wait_recv()
        xcopy(cc, ym, other, 0, 13 + s // 2, to_pt).wait_recv()
        xcopy(cc, yp, other, 0, 14 + s // 2, to_pt).wait_recv()
        xcopy(cc, yo, other, 0, 15 + s // 2, to_pt).wait_recv()

    for load in loads0:
        load.wait()
    wx0(0)
    wz0(0, 0)
    for load in loadx:
        load.wait()

    def prenorm(i, carry):
        rows = pl.ds(pl.multiple_of(i * 16, 16), 16)
        h = hid[rows, :].astype(F32)
        r = lax.rsqrt(jnp.mean(h * h, axis=-1, keepdims=True) + EPSILON)
        to = pl.ds(pl.multiple_of(b * TOK + t * SUB + i * 16, 16), 16)
        xs[to, :] = (h * r * pre[...]).astype(BF)
        return carry

    lax.fori_loop(0, SUB // 16, prenorm, 0)
    xcopy(b, y, core, 0, 0, to_xq).start()
    xsend0(b, 0)
    for load in loads1:
        load.wait()
    wx0(1)
    wx1(0)
    wz1(0)
    wz2(0)
    for load in loads2:
        load.wait()
    wfwd(0, 0)
    xcopy(nb, y, core, 0, 0, to_xq).wait_recv()
    xsend0(nb, 6)
    wx1(1)
    wfwd(0, 1)
    wfwd(0, 2)
    wz0(1, 0)

    base = WINDOW + (c - b) * TOK

    def angle(i, carry):
        rows = pl.ds(pl.multiple_of(i * 128, 128), 128)
        pos = lax.broadcasted_iota(jnp.int32, (128, HD), 0) + (base + i * 128)
        a = pos.astype(F32) * freq_v[...]
        lane = lax.broadcasted_iota(jnp.int32, (128, HD), 1)
        cos[rows, :] = jnp.cos(a)
        sn = jnp.sin(a)
        sin[rows, :] = jnp.where(lane < HD // 2, -sn, sn)
        return carry

    lax.fori_loop(0, PAIR // 128, angle, 0)
    xhop(b, 0)
    wfwd(0, 3)
    wz1(1)
    wz2(1)
    o0(0)
    o0s(1)
    wlast(0)
    wfwd(1, 0)
    o1(0)
    wfwd(1, 1)
    wfwd(1, 2)
    xhop(nb, 6)
    wfwd(1, 3)
    o0(1)
    o0s(0)
    o1s(0)
    o3(0)
    xopp(b, 0)
    xdone(b, 0)
    wlast(1)
    o1(1)
    xopp(nb, 6)
    xdone(nb, 6)

    def mm(w):
        def step(i, carry):
            ks = pl.ds(pl.multiple_of(i * KT, 128), KT)
            acc[...] += jnp.dot(xs[:, ks], w[ks, :], preferred_element_type=F32)
            return carry

        acc[...] = jnp.zeros((PAIR, 256), F32)
        lax.fori_loop(0, D // KT, step, 0)

    def headed(rows, c0, gain):
        raw = acc[rows, c0:c0 + HD]
        r = lax.rsqrt(jnp.mean(raw * raw, axis=-1, keepdims=True) + EPSILON)
        n = raw * r * gain[...]
        return n * cos[rows, :] + pltpu.roll(n, HD // 2, 1) * sin[rows, :]

    def keys(i, carry):
        rows = pl.ds(pl.multiple_of(i * 128, 128), 128)
        to = pl.ds(pl.multiple_of(WINDOW + i * 128, 128), 128)
        kv[0, to, :] = headed(rows, 0, kg_v).astype(BF)
        kv[1, to, :] = acc[rows, HD:2 * HD].astype(BF)
        return carry

    def queries(i, carry):
        rows = pl.ds(pl.multiple_of(i * 128, 128), 128)
        for h in range(2):
            qb[h, rows, :] = (headed(rows, h * HD, qg_v) * QUERY_FACTOR).astype(BF)
        return carry

    def kcopy(half, i, to):
        return remote(
            kv.at[i, pl.ds(WINDOW + half * TOK, TOK), :], kr.at[half, i],
            krsend.at[half, i], krrecv.at[half, i], to,
        )

    def kfinal(half, i, to):
        return remote(
            kr.at[half, i], kv.at[i, pl.ds(half * TOK, TOK), :],
            kfsend.at[half, i], kfrecv.at[half, i], to,
        )

    mm(w0)
    for half in range(2):
        lax.fori_loop(4 * half, 4 * half + 4, keys, 0)

        @pl.when(c < 14)
        def _():
            for i in range(2):
                kcopy(half, i, (to_xq, to_xn)[half]).start()

    o1s(1)
    o3(1)
    mm(w1)

    def onward(half):
        src = (cq, cn)[half]

        @pl.when(src < 14)
        def _():
            for i in range(2):
                kcopy(half, i, to_xq).wait_recv()
                kfinal(half, i, dev((src + 2) % 16)).start()

    onward(0)
    onward(1)
    lax.fori_loop(0, 8, queries, 0)
    for col in range(2):
        ofwd(col, 0)

    @pl.when(c < 2)
    def _():
        prior(0).wait()
        prior(1).wait()

    @pl.when(c >= 2)
    def _():
        for half in range(2):
            for i in range(2):
                kfinal(half, i, to_xq).wait_recv()

    first = WINDOW - start_s[0] - (c - b) * TOK

    def attend(q0):
        q = qb[:, pl.ds(q0, 128), :].reshape(256, HD)
        k = kv[0, pl.ds(q0, 1152), :]
        v = kv[1, pl.ds(q0, 1152), :]
        s = lax.dot_general(q, k, (((1,), (1,)), ((), ())), preferred_element_type=F32)
        j = lax.broadcasted_iota(jnp.int32, (256, 1152), 1)
        r = lax.broadcasted_iota(jnp.int32, (256, 1152), 0)
        r = jnp.where(r >= 128, r - 128, r)
        s = jnp.where((j > r) & (j <= r + WINDOW) & (j >= first - q0), s, F32(-1e30))
        m = jnp.max(s, axis=-1, keepdims=True)
        e = jnp.exp(s - m)
        total = jnp.sum(e, axis=-1, keepdims=True)
        return (jnp.dot(e.astype(BF), v, preferred_element_type=F32) / total).astype(BF)

    def swap(i):
        rows = pl.ds(pl.multiple_of(i * 128, 128), 128)
        return remote(ast.at[rows, :], att.at[b, rows, :], swsend.at[i], swrecv.at[i], to_xq)

    def unit_pair(i, carry):
        o = attend(pl.multiple_of(nb * TOK + i * 128, 128))
        rows = pl.ds(pl.multiple_of(i * 128, 128), 128)
        ast[rows, 0:128] = o[:128]
        ast[rows, 128:256] = o[128:]
        swap(i).start()
        return carry

    def unit_own(i, carry):
        o = attend(pl.multiple_of(b * TOK + i * 128, 128))
        rows = pl.ds(pl.multiple_of(i * 128, 128), 128)
        att[b, rows, 0:128] = o[:128]
        att[b, rows, 128:256] = o[128:]
        return carry

    lax.fori_loop(0, 4, unit_pair, 0)
    for col in range(2):
        ofwd(col, 1)
        ofwd(col, 2)
    lax.fori_loop(0, 4, unit_own, 0)
    for i in range(4):
        rows = pl.ds(i * 128, 128)
        remote(ast.at[rows, :], att.at[nb, rows, :], swsend.at[i], swrecv.at[i], to_xq).wait_recv()

    CHUNKS = [(0, 0), (1, 0), (0, 1), (0, 2), (1, 1), (1, 2), (0, 3), (1, 3)]

    def at_s(q):
        col, j = CHUNKS[q]
        return nxt(fs(col)[1], JF[j])

    def wide(q):
        return pl.ds(0, CWP[CHUNKS[q][0]])

    def rcopy(src, dst, q, sem, to):
        return remote(src, dst, rsend.at[q, sem], rrecv.at[q, sem], to)

    def r0copy(q):
        return rcopy(pp.at[q, :, other, :, wide(q)], dd.at[q, :, :, wide(q)], q, 0, to_pt)

    def r1copy(q, half):
        return rcopy(
            cb.at[q, 0, pl.ds(half * 32, 32), wide(q)], ee.at[q, half, :, wide(q)], q, 1 + half,
            (to_yp, to_ym)[half],
        )

    def r2copy(q, half):
        return rcopy(
            cb.at[q, 1 + half, :, wide(q)], gg.at[q, half, :, wide(q)], q, 3 + half,
            (to_yp, to_ym)[half],
        )

    def proj(q):
        col = CHUNKS[q][0]
        n = CW[col]
        wref = (oa, ob)[col]
        rows = pl.ds(pl.multiple_of(at_s(q) * n, 16), n)

        def part(i, carry):
            tok = pl.ds(pl.multiple_of(i * 256, 256), 256)
            o = None
            for h in range(2):
                d = lax.dot_general(
                    att[h, tok, :], wref[rows, h * 256:(h + 1) * 256],
                    (((1,), (1,)), ((), ())), preferred_element_type=F32,
                )
                o = d if o is None else o + d
            o = o.astype(BF)
            for g in range(4):
                pp[q, i * 2 + g // 2, g % 2, :, 0:n] = o[g * SUB:(g + 1) * SUB]
            return carry

        lax.fori_loop(0, 2, part, 0)
        r0copy(q).start()

    def both(q, yy):
        w = CWP[CHUNKS[q][0]]
        return pp[q, yy, core, :, 0:w].astype(F32) + dd[q, yy, :, 0:w].astype(F32)

    def r1(q):
        w = CWP[CHUNKS[q][0]]
        r0copy(q).wait_recv()
        cb[q, 0, :, 0:w] = both(q, yo).astype(BF)
        r1copy(q, 0).start()
        r1copy(q, 1).start()

    def r2(q):
        w = CWP[CHUNKS[q][0]]
        r1copy(q, 0).wait_recv()
        a = both(q, yp)
        cb[q, 1, 0:32, 0:w] = (a[0:32] + ee[q, 0, :, 0:w].astype(F32)).astype(BF)
        cb[q, 1, 32:64, 0:w] = a[32:64].astype(BF)
        r2copy(q, 0).start()
        r1copy(q, 1).wait_recv()
        a = both(q, ym)
        cb[q, 2, 0:32, 0:w] = a[0:32].astype(BF)
        cb[q, 2, 32:64, 0:w] = (a[32:64] + ee[q, 1, :, 0:w].astype(F32)).astype(BF)
        r2copy(q, 1).start()

    def r3(q):
        w = CWP[CHUNKS[q][0]]
        r2copy(q, 0).wait_recv()
        r2copy(q, 1).wait_recv()
        v = both(q, y) + gg[q, 0, :, 0:w].astype(F32) + gg[q, 1, :, 0:w].astype(F32)
        (sa, sb)[CHUNKS[q][0]][at_s(q)] = v

    for q in range(8):
        if CHUNKS[q][0] == 0:
            for g in range(8):
                pp[q, g // 2, g % 2, :, 512:640] = jnp.zeros((SUB, 128), BF)

    proj(0)
    proj(1)
    r1(0)
    r1(1)
    for col in range(2):
        ofwd(col, 3)
    proj(2)
    r2(0)
    proj(3)
    r2(1)
    r1(2)
    r1(3)
    proj(4)
    proj(5)
    r2(2)
    r2(3)
    r1(4)
    r1(5)
    olast(0)
    proj(6)
    r3(0)
    r3(1)
    r2(4)
    r1(6)
    olast(1)
    proj(7)
    r2(5)
    r3(2)
    r1(7)
    r3(3)
    r2(6)
    r3(4)
    r2(7)
    r3(5)
    r3(6)
    r3(7)

    for i in range(16):
        zi, xi = i // 4, i % 4
        full[:, i * BLK:i * BLK + ON[0]] = sa[zi, :, xi * ON[0]:(xi + 1) * ON[0]]
        full[:, i * BLK + ON[0]:(i + 1) * BLK] = sb[xi, :, zi * ON[1]:(zi + 1) * ON[1]]

    def final(i, carry):
        rows = pl.ds(pl.multiple_of(i * 16, 16), 16)
        v = full[rows, :]
        r = lax.rsqrt(jnp.mean(v * v, axis=-1, keepdims=True) + EPSILON)
        out_v[rows, :] = (hid[rows, :].astype(F32) + v * r * post[...]).astype(BF)
        return carry

    lax.fori_loop(0, SUB // 16, final, 0)

    for p in range(2):
        remote(ws[p], ws[p], wsend.at[p], wrecv.at[p, 0], to_pt).wait_send()
    for col in range(2):
        ref = (oa, ob)[col].at[pl.ds(0, 15 * ON[col]), :]
        remote(ref, ref, osend.at[col], orecv.at[col, 0], to_pt).wait_send()
    ref = xs.at[pl.ds(0, 15 * SUB), :]
    remote(ref, ref, xsend, xrecv.at[0], to_pt).wait_send()
    for half in range(2):

        @pl.when(c < 14)
        def _():
            for i in range(2):
                kcopy(half, i, to_xq).wait_send()

        @pl.when((cq, cn)[half] < 14)
        def _():
            for i in range(2):
                kfinal(half, i, to_xq).wait_send()

    for i in range(4):
        swap(i).wait_send()
    for q in range(8):
        r0copy(q).wait_send()
        for half in range(2):
            r1copy(q, half).wait_send()
            r2copy(q, half).wait_send()


def local(
    hidden_in, stretch_start, pre_gain, q_weight, k_weight, v_weight, o_weight, q_gain, k_gain,
    prior_keys, prior_values, post_gain,
):
    frequency = 10000.0 ** (-jnp.arange(HD // 2, dtype=F32) / (HD // 2))
    freq2 = jnp.concatenate([frequency, frequency]).reshape(1, HD)
    hbm = pl.BlockSpec(memory_space=pl.ANY)
    vm = pl.BlockSpec(memory_space=pltpu.VMEM)
    sm = pl.BlockSpec(memory_space=pltpu.SMEM)
    dma = pltpu.SemaphoreType.DMA
    return pl.pallas_call(
        body,
        out_shape=jax.ShapeDtypeStruct((SUB, D), BF),
        in_specs=[hbm, sm, hbm, hbm, hbm, hbm, hbm, vm, vm, hbm, hbm, hbm, vm],
        out_specs=vm,
        scratch_shapes=[
            pltpu.VMEM((D, 256), BF), pltpu.VMEM((D, 256), BF),
            pltpu.VMEM((16 * ON[0], 512), BF), pltpu.VMEM((16 * ON[1], 512), BF),
            pltpu.VMEM((2, 2, BLK, 256), BF), pltpu.VMEM((2, 2, 176, 256), BF),
            pltpu.VMEM((PAIR, D), BF),
            pltpu.VMEM((2, WINDOW + PAIR, HD), BF), pltpu.VMEM((2, 2, TOK, HD), BF),
            pltpu.VMEM((2, PAIR, HD), BF),
            pltpu.VMEM((2, TOK, 256), BF), pltpu.VMEM((TOK, 256), BF),
            pltpu.VMEM((PAIR, 256), F32),
            pltpu.VMEM((SUB, D), BF), pltpu.VMEM((1, D), F32), pltpu.VMEM((1, D), F32),
            pltpu.VMEM((PAIR, HD), F32), pltpu.VMEM((PAIR, HD), F32),
            pltpu.VMEM((8, 4, 2, SUB, 768), BF),
            pltpu.VMEM((8, 4, SUB, 768), BF),
            pltpu.VMEM((8, 2, SUB // 2, 768), BF),
            pltpu.VMEM((8, 2, SUB, 768), BF),
            pltpu.VMEM((8, 3, SUB, 768), BF),
            pltpu.VMEM((4, SUB, CWP[0]), F32), pltpu.VMEM((4, SUB, CWP[1]), F32),
            pltpu.VMEM((SUB, D), F32),
            dma((16,)), dma((2,)), dma((2, 22)), dma((2,)), dma((2, 20)), dma, dma((20,)),
            dma((2, 2)), dma((2, 2)), dma((2, 2)), dma((2, 2)), dma((4,)), dma((4,)),
            dma((8, 5)), dma((8, 5)),
        ],
        compiler_params=pltpu.CompilerParams(
            collective_id=0, has_side_effects=True, vmem_limit_bytes=64 * 1024 * 1024 - 128 * 1024
        ),
        name="layer",
    )(
        hidden_in, stretch_start, pre_gain, q_weight, k_weight, v_weight,
        o_weight.T, q_gain.reshape(1, HD), k_gain.reshape(1, HD), prior_keys, prior_values,
        post_gain, freq2,
    )


def solution(mesh):
    return jax.shard_map(
        local,
        mesh=mesh,
        in_specs=(
            P(("ctx", "tp"), None), P(), P(), P("ctx", "tp"), P("ctx", "tp"), P("ctx", "tp"),
            P("tp", "ctx"), P(), P(), P(None, "tp"), P(None, "tp"), P(),
        ),
        out_specs=P(("ctx", "tp"), None),
        check_vma=False,
    )
```

```python
import jax
import jax.numpy as jnp
from jax import lax
from jax.experimental import pallas as pl
from jax.experimental.pallas import tpu as pltpu
from jax.sharding import PartitionSpec as P

HD = 128
WINDOW = 1024
EPSILON = 1e-06
QUERY_FACTOR = 168.0 ** (-0.5)
MESH = pl.DeviceIdType.MESH

D = 5376
BLK = 336
TOK = 512
PAIR = 1024
SUB = 64
HALF = (0, 336), (0, 176), (176, 160)
ON = (144, 192)
OH = ((0, 144), (0, 80), (80, 64)), ((0, 192), (0, 96), (96, 96))
CW = (576, 768)
CWP = (640, 768)
KT = 768
BF = jnp.bfloat16
F32 = jnp.float32
ORDER = (
    "wr,0", "ww,0", "wz0,0", "pn", "xp,1", "xo,0", "xo,1", "xp,0", "wf,0,1", "wf,0,0", "wr,1", "ww,1", "wfw,0,0,0", "wfw,0,0,1", "wzx,0,2",
    "wzx,0,1", "os,0,0,0", "os,0,0,1", "xf,0,0", "wf,1,1", "ang", "zero", "wzx,1,2", "wfw,0,2,0", "wfw,0,2,1", "xg,1", "wfw,0,1,1",
    "wfw,0,1,0", "xm,0,0", "xf,0,1", "xm,0,1", "xg,0", "wfw,1,2,1", "wfw,1,2,0", "wzo,0", "xf,1,1", "wf,1,0", "wz0,1", "wzx,1,1", "wzo,1",
    "wfw,0,3,1", "xopp,0", "wfw,0,3,0", "xd,0", "os,1,0,0", "os,1,0,1", "wfw,1,0,1", "wfw,1,0,0", "of,0,0,0", "of,0,0,1",
    "wfw,1,1,1", "o0,0,0", "o0,0,1", "xf,1,0", "xm,1,0", "xm,1,1", "wfw,1,1,0", "of,1,0,0", "of,1,0,1", "wfw,1,3,1", "wfw,1,3,0",
    "o1,0,0", "o1,0,1", "os,0,1,0", "os,0,2,0", "os,0,1,1", "os,0,2,1", "wl,0", "mk,0", "o0,1,0", "o0,1,1", "o3,0", "os,0,3,0", "os,0,3,1",
    "xopp,1", "xd,1", "mk,1", "kvf,0,0", "kvf,0,1", "wl,1", "mq,0", "of,0,1,1", "mq,1", "kvf,1,0", "kvf,1,1", "of,0,1,0", "of,0,2,1",
    "of,0,2,0", "o1,1,1", "os,1,2,0", "os,1,2,1", "aw", "au,0", "au,1", "au,2", "au,3", "of,0,3,0", "of,0,3,1", "ao,0", "ao,1", "of,1,2,0",
    "of,1,2,1", "ao,2", "ao,3", "o1,1,0", "os,1,1,0", "os,1,1,1", "sw", "pj,0", "pj,2", "pj,3", "r1,0", "pj,6", "r1,2", "of,1,1,1", "o3,1",
    "os,1,3,0", "os,1,3,1", "pj,1", "r1,3", "r1,6", "r2,0,0", "r2,0,1", "r1,1", "r2,2,0", "r2,2,1", "of,1,1,0", "r2,3,0", "r2,3,1", "r2,6,0",
    "r2,6,1", "r3,0", "of,1,3,0", "pj,4", "r2,1,0", "r2,1,1", "of,1,3,1", "pj,5", "r3,2", "r1,4", "r1,5", "r3,3", "pj,7", "r3,6", "r1,7", "r3,1",
    "r2,4,0", "r2,4,1", "r2,5,0", "r2,5,1", "r2,7,0", "r2,7,1", "r3,4", "r3,5", "r3,7",
)


def body(
    hid_h, start_s, pre_h, q_h, k_h, v_h, o_h, qg_v, kg_v, pk_h, pv_h, post_h, freq_v,
    out_v,
    w0, w1, oa, ob, ow, rb, xs, kv, kr, qb, att, ast, acc, hid, pre, post, cos, sin,
    pp, dd, ee, gg, cb, sa, sb, full,
    lsem, wsend, wrecv, osend, orecv, xsend, xrecv, krsend, krrecv, kfsend, kfrecv,
    swsend, swrecv, rsend, rrecv,
):
    c = lax.axis_index("ctx")
    t = lax.axis_index("tp")
    z, x = c // 4, c % 4
    y, core = t // 2, t % 2
    b = x % 2
    nb = 1 - b
    ws = (w0, w1)

    def nxt(a, d):
        return (a + d + 4) % 4

    def pairx(xx):
        return xx + 1 - 2 * (xx % 2)

    def otherx(xx):
        return (xx + 3 + 2 * (xx % 2)) % 4

    xq, xn, xo = pairx(x), otherx(x), nxt(x, 2)
    yp, ym, yo = nxt(y, 1), nxt(y, -1), nxt(y, 2)
    other = 1 - core
    to_yp = {"ctx": c, "tp": yp * 2 + core}
    to_ym = {"ctx": c, "tp": ym * 2 + core}
    to_pt = {"ctx": c, "tp": y * 2 + other}

    def dev(ci):
        return {"ctx": ci, "tp": t}

    to_xq, to_xn = dev(z * 4 + xq), dev(z * 4 + xn)
    to_zp, to_zm = dev(nxt(z, 1) * 4 + x), dev(nxt(z, -1) * 4 + x)

    def remote(src, dst, ssem, rsem, to):
        return pltpu.make_async_remote_copy(
            src_ref=src, dst_ref=dst, send_sem=ssem, recv_sem=rsem, device_id=to,
            device_id_type=MESH,
        )

    own = pl.ds(pl.multiple_of(c * BLK, 16), BLK)
    hc = pl.ds(pl.multiple_of(b * HD, HD), HD)
    lo, hi = pl.ds(0, HD), pl.ds(HD, HD)
    loads0 = [
        pltpu.make_async_copy(k_h.at[:, lo], ow.at[0, 0, :, lo], lsem.at[0]),
        pltpu.make_async_copy(v_h.at[:, lo], ow.at[0, 0, :, hi], lsem.at[1]),
        pltpu.make_async_copy(k_h.at[:, hi], ow.at[0, 1, :, lo], lsem.at[2]),
        pltpu.make_async_copy(v_h.at[:, hi], ow.at[0, 1, :, hi], lsem.at[3]),
        pltpu.make_async_copy(k_h.at[:, hc], w0.at[own, lo], lsem.at[4]),
        pltpu.make_async_copy(v_h.at[:, hc], w0.at[own, hi], lsem.at[5]),
    ]
    loadx = [
        pltpu.make_async_copy(hid_h, hid, lsem.at[6]),
        pltpu.make_async_copy(pre_h, pre.at[0], lsem.at[7]),
    ]
    loads1 = [
        pltpu.make_async_copy(q_h.at[:, pl.ds(0, 256)], ow.at[1, 0], lsem.at[8]),
        pltpu.make_async_copy(q_h.at[:, pl.ds(256, 256)], ow.at[1, 1], lsem.at[9]),
        pltpu.make_async_copy(
            q_h.at[:, pl.ds(pl.multiple_of(b * 256, 256), 256)], w1.at[own, :], lsem.at[10]
        ),
    ]
    loads2 = [
        pltpu.make_async_copy(
            o_h.at[pl.ds(0, ON[0]), :],
            oa.at[pl.ds(pl.multiple_of(c * ON[0], 16), ON[0]), :], lsem.at[11],
        ),
        pltpu.make_async_copy(
            o_h.at[pl.ds(ON[0], ON[1]), :],
            ob.at[pl.ds(pl.multiple_of((x * 4 + z) * ON[1], 16), ON[1]), :], lsem.at[12],
        ),
        pltpu.make_async_copy(post_h, post.at[0], lsem.at[13]),
    ]
    for load in loads0 + loadx + loads1 + loads2:
        load.start()

    def prior(i):
        return pltpu.make_async_copy(
            (pk_h, pv_h)[i].at[:, hc], kv.at[i, pl.ds(0, WINDOW), :], lsem.at[14 + i]
        )

    @pl.when(c < 2)
    def _():
        prior(0).start()
        prior(1).start()

    cq, cn = z * 4 + xq, z * 4 + xn
    behind = (c + 14) % 16
    zb, xb = behind // 4, behind % 4
    barrier = pltpu.get_barrier_semaphore()
    peers = [to_yp, to_ym, to_pt, to_xq, to_xn, to_zp, to_zm]
    peers += [dev((cq + 2) % 16), dev((cn + 2) % 16)]
    peers += [dev(zb * 4 + pairx(xb)), dev(zb * 4 + otherx(xb))]
    for peer in peers:
        pl.semaphore_signal(barrier, inc=1, device_id=peer, device_id_type=MESH)
    pl.semaphore_wait(barrier, len(peers))

    steps = {}

    def step(fn):
        steps[fn.__name__[1:]] = fn
        return fn

    waited = set()

    def need(name, group):
        if name not in waited:
            waited.add(name)
            for load in group:
                load.wait()

    def need_w(p):
        need(p, (loads0, loads1)[p])

    XJ = (x, xq, xn, xo)
    to_z = (to_zp, to_zm)

    def wrows(zz, xx, part):
        off, num = HALF[part]
        return pl.ds(pl.multiple_of((zz * 4 + xx) * BLK + off, 16), num)

    def wx(p, src, xx, part, sem, to):
        return remote(
            src, ws[p].at[wrows(z, xx, part), :], wsend.at[p], wrecv.at[p, sem], to
        )

    def wz(p, zz, j, part, sem, to):
        ref = ws[p].at[wrows(zz, XJ[j], part), :]
        return remote(ref, ref, wsend.at[p], wrecv.at[p, sem], to)

    def relay_in(p, side):
        off, num = HALF[1 + side]
        return remote(
            ow.at[p, b, pl.ds(off, num), :], rb.at[p, side, pl.ds(0, num), :],
            wsend.at[p], wrecv.at[p, 2 + side], (to_xq, to_xn)[side],
        )

    def relay_out(p, side, xx):
        src = rb.at[p, side, pl.ds(0, HALF[1 + side][1]), :]
        return wx(p, src, xx, 1 + side, 4 + side, (to_xn, to_xq)[side])

    def whole(p, side, xx):
        return wx(p, ow.at[p, nb], xx, 0, side, (to_xq, to_xn)[side])

    def wz_out(p, j):
        for i in range(2):
            wz(p, z, j, 0, 6 + 2 * j + i, to_z[i]).start()

    @step
    def _wr(p):
        need_w(p)
        relay_in(p, 0).start()
        relay_in(p, 1).start()

    @step
    def _ww(p):
        need_w(p)
        whole(p, 0, x).start()
        whole(p, 1, x).start()

    @step
    def _wz0(p):
        need_w(p)
        wz_out(p, 0)

    @step
    def _wf(p, side):
        relay_in(p, side).wait_recv()
        relay_out(p, side, (xq, xn)[side]).start()

    @step
    def _wzx(p, j):
        whole(p, j - 1, XJ[j]).wait_recv()
        wz_out(p, j)

    @step
    def _wzo(p):
        relay_out(p, 0, xo).wait_recv()
        relay_out(p, 1, xo).wait_recv()
        wz_out(p, 3)

    @step
    def _wfw(p, j, i):
        zz = nxt(z, (-1, 1)[i])
        wz(p, zz, j, 0, 6 + 2 * j + i, to_z[i]).wait_recv()
        wz(p, zz, j, 1 + i, 14 + 2 * j + i, to_z[i]).start()

    @step
    def _wl(p):
        for j in range(4):
            for i in range(2):
                wz(p, nxt(z, 2), j, 1 + i, 14 + 2 * j + i, to_z[i]).wait_recv()

    JF = (0, -1, 1, 2)

    def fs(col):
        return (x, z) if col == 0 else (z, x)

    def ctx_of(col, f, s):
        return s * 4 + f if col == 0 else f * 4 + s

    def ocopy(col, fj, sj, part, sem, df, ds):
        f0, s0 = fs(col)
        off, num = OH[col][part]
        f, s = nxt(f0, fj), nxt(s0, sj)
        ref = (oa, ob)[col].at[pl.ds(pl.multiple_of((s * 4 + f) * ON[col] + off, 16), num), :]
        to = dev(ctx_of(col, nxt(f0, df), nxt(s0, ds)))
        return remote(ref, ref, osend.at[col], orecv.at[col, sem], to)

    WAY = (1, -1)

    @step
    def _o0(col, i):
        need(2, loads2)
        ocopy(col, 0, 0, 0, i, WAY[i], 0).start()

    @step
    def _o1(col, i):
        ocopy(col, -WAY[i], 0, 0, i, WAY[i], 0).wait_recv()
        ocopy(col, -WAY[i], 0, 1 + i, 2 + i, WAY[i], 0).start()

    @step
    def _o3(col):
        ocopy(col, 2, 0, 1, 2, 1, 0).wait_recv()
        ocopy(col, 2, 0, 2, 3, 1, 0).wait_recv()

    @step
    def _os(col, j, i):
        need(2, loads2)
        ocopy(col, JF[j], 0, 0, 4 + 2 * j + i, 0, WAY[i]).start()

    @step
    def _of(col, j, i):
        ocopy(col, JF[j], -WAY[i], 0, 4 + 2 * j + i, 0, WAY[i]).wait_recv()
        ocopy(col, JF[j], -WAY[i], 1 + i, 12 + 2 * j + i, 0, WAY[i]).start()

    CC = (b, nb)

    def xcopy(cc, yy, kk, part, sem, to):
        off, num = ((0, SUB), (0, SUB // 2), (SUB // 2, SUB // 2))[part]
        row = CC[cc] * TOK + (yy * 2 + kk) * SUB + off
        ref = xs.at[pl.ds(pl.multiple_of(row, 16), num), :]
        return remote(ref, ref, xsend, xrecv.at[sem], to)

    to_y = (to_yp, to_ym)

    def xsem(cc, k):
        return cc * 11 + k

    @step
    def _pn():
        need("x", loadx)

        def prenorm(i, carry):
            rows = pl.ds(pl.multiple_of(i * 16, 16), 16)
            h = hid[rows, :].astype(F32)
            r = lax.rsqrt(jnp.mean(h * h, axis=-1, keepdims=True) + EPSILON)
            to = pl.ds(pl.multiple_of(b * TOK + t * SUB + i * 16, 16), 16)
            xs[to, :] = (h * r * pre[...]).astype(BF)
            return carry

        lax.fori_loop(0, SUB // 16, prenorm, 0)

    @step
    def _xp(h):
        xcopy(0, y, core, 1 + h, 22 + h, to_xq).start()

    def xout(cc, h):
        for i in range(2):
            xcopy(cc, y, core, 1 + h, xsem(cc, 2 * i + h), to_y[i]).start()
        xcopy(cc, y, core, 1 + h, xsem(cc, 6 + h), to_pt).start()

    @step
    def _xo(h):
        xout(0, h)

    @step
    def _xg(h):
        xcopy(1, y, core, 1 + h, 22 + h, to_xq).wait_recv()
        xout(1, h)

    YB = (ym, yp)

    @step
    def _xf(cc, i):
        xcopy(cc, YB[i], core, 1 + i, xsem(cc, 3 * i), to_y[i]).wait_recv()
        xcopy(cc, YB[i], core, 1 + i, xsem(cc, 4 + i), to_y[i]).start()

    @step
    def _xm(cc, i):
        xcopy(cc, YB[i], core, 2 - i, xsem(cc, 1 + i), to_y[i]).wait_recv()
        xcopy(cc, YB[i], core, 0, xsem(cc, 8 + i), to_pt).start()

    @step
    def _xopp(cc):
        xcopy(cc, yo, core, 1, xsem(cc, 4), to_yp).wait_recv()
        xcopy(cc, yo, core, 2, xsem(cc, 5), to_ym).wait_recv()
        xcopy(cc, yo, core, 0, xsem(cc, 10), to_pt).start()

    @step
    def _xd(cc):
        xcopy(cc, y, other, 1, xsem(cc, 6), to_pt).wait_recv()
        xcopy(cc, y, other, 2, xsem(cc, 7), to_pt).wait_recv()
        xcopy(cc, ym, other, 0, xsem(cc, 8), to_pt).wait_recv()
        xcopy(cc, yp, other, 0, xsem(cc, 9), to_pt).wait_recv()
        xcopy(cc, yo, other, 0, xsem(cc, 10), to_pt).wait_recv()

    base = WINDOW + (c - b) * TOK

    @step
    def _ang():
        def angle(i, carry):
            rows = pl.ds(pl.multiple_of(i * 128, 128), 128)
            pos = lax.broadcasted_iota(jnp.int32, (128, HD), 0) + (base + i * 128)
            a = pos.astype(F32) * freq_v[...]
            lane = lax.broadcasted_iota(jnp.int32, (128, HD), 1)
            cos[rows, :] = jnp.cos(a)
            sn = jnp.sin(a)
            sin[rows, :] = jnp.where(lane < HD // 2, -sn, sn)
            return carry

        lax.fori_loop(0, PAIR // 128, angle, 0)

    def mm(w, cc):
        def part(i, carry):
            ks = pl.ds(pl.multiple_of(i * KT, 128), KT)
            rows = pl.ds(pl.multiple_of(CC[cc] * TOK, TOK), TOK)
            acc[...] += jnp.dot(xs[rows, ks], w[ks, :], preferred_element_type=F32)
            return carry

        acc[...] = jnp.zeros((TOK, 256), F32)
        lax.fori_loop(0, D // KT, part, 0)

    def headed(i, cc, c0, gain):
        raw = acc[pl.ds(pl.multiple_of(i * 128, 128), 128), c0:c0 + HD]
        at = pl.ds(pl.multiple_of(CC[cc] * TOK + i * 128, 128), 128)
        r = lax.rsqrt(jnp.mean(raw * raw, axis=-1, keepdims=True) + EPSILON)
        n = raw * r * gain[...]
        return n * cos[at, :] + pltpu.roll(n, HD // 2, 1) * sin[at, :]

    def kcopy(cc, i):
        rows = pl.ds(pl.multiple_of(WINDOW + CC[cc] * TOK, TOK), TOK)
        return remote(
            kv.at[i, rows, :], kr.at[cc, i], krsend.at[cc, i], krrecv.at[cc, i],
            (to_xq, to_xn)[i],
        )

    def kfinal(cc, i, half, to):
        rows = pl.ds(pl.multiple_of(half * TOK, TOK), TOK)
        return remote(
            kr.at[cc, i], kv.at[i, rows, :], kfsend.at[cc, i], kfrecv.at[cc, i], to
        )

    @step
    def _mk(cc):
        mm(w0, cc)

        def keys(i, carry):
            rows = pl.ds(pl.multiple_of(i * 128, 128), 128)
            to = pl.ds(pl.multiple_of(WINDOW + CC[cc] * TOK + i * 128, 128), 128)
            kv[0, to, :] = headed(i, cc, 0, kg_v).astype(BF)
            kv[1, to, :] = acc[rows, HD:2 * HD].astype(BF)
            return carry

        lax.fori_loop(0, 4, keys, 0)

        @pl.when(c < 14)
        def _():
            kcopy(cc, 0).start()
            kcopy(cc, 1).start()

    @step
    def _kvf(cc, i):
        src = (cq, cn)[i]

        @pl.when(src < 14)
        def _():
            kcopy(cc, i).wait_recv()
            kfinal(cc, i, CC[1 - cc], dev((src + 2) % 16)).start()

    @step
    def _mq(cc):
        mm(w1, cc)

        def queries(i, carry):
            to = pl.ds(pl.multiple_of(CC[cc] * TOK + i * 128, 128), 128)
            for h in range(2):
                qb[h, to, :] = (headed(i, cc, h * HD, qg_v) * QUERY_FACTOR).astype(BF)
            return carry

        lax.fori_loop(0, 4, queries, 0)

    @step
    def _aw():
        @pl.when(c < 2)
        def _():
            prior(0).wait()
            prior(1).wait()

        @pl.when(c >= 2)
        def _():
            for cc in range(2):
                for i in range(2):
                    kfinal(cc, i, CC[cc], to_xq).wait_recv()

    first = WINDOW - start_s[0] - (c - b) * TOK

    def attend(q0):
        q = qb[:, pl.ds(q0, 128), :].reshape(256, HD)
        k = kv[0, pl.ds(q0, 1152), :]
        v = kv[1, pl.ds(q0, 1152), :]
        s = lax.dot_general(q, k, (((1,), (1,)), ((), ())), preferred_element_type=F32)
        j = lax.broadcasted_iota(jnp.int32, (256, 1152), 1)
        r = lax.broadcasted_iota(jnp.int32, (256, 1152), 0)
        r = jnp.where(r >= 128, r - 128, r)
        s = jnp.where((j > r) & (j <= r + WINDOW) & (j >= first - q0), s, F32(-1e30))
        m = jnp.max(s, axis=-1, keepdims=True)
        e = jnp.exp(s - m)
        total = jnp.sum(e, axis=-1, keepdims=True)
        return (jnp.dot(e.astype(BF), v, preferred_element_type=F32) / total).astype(BF)

    def swap(i, from_pair):
        rows = pl.ds(i * 128, 128)
        half = nb if from_pair else b
        return remote(ast.at[rows, :], att.at[half, rows, :], swsend.at[i], swrecv.at[i], to_xq)

    @step
    def _au(i):
        o = attend(pl.multiple_of(nb * TOK + i * 128, 128))
        ast[i * 128:(i + 1) * 128, 0:128] = o[:128]
        ast[i * 128:(i + 1) * 128, 128:256] = o[128:]
        swap(i, False).start()

    @step
    def _ao(i):
        o = attend(pl.multiple_of(b * TOK + i * 128, 128))
        att[b, i * 128:(i + 1) * 128, 0:128] = o[:128]
        att[b, i * 128:(i + 1) * 128, 128:256] = o[128:]

    @step
    def _sw():
        for i in range(4):
            swap(i, True).wait_recv()

    CHUNKS = [(0, 0), (1, 0), (0, 1), (0, 2), (1, 1), (1, 2), (0, 3), (1, 3)]

    def at_s(q):
        col, j = CHUNKS[q]
        return nxt(fs(col)[1], JF[j])

    def wide(q):
        return pl.ds(0, CWP[CHUNKS[q][0]])

    def rcopy(src, dst, q, sem, to):
        return remote(src, dst, rsend.at[q, sem], rrecv.at[q, sem], to)

    def r0copy(q):
        return rcopy(pp.at[q, :, other, :, wide(q)], dd.at[q, :, :, wide(q)], q, 0, to_pt)

    def r1copy(q, half):
        return rcopy(
            cb.at[q, 0, pl.ds(half * 32, 32), wide(q)], ee.at[q, half, :, wide(q)], q, 1 + half,
            to_y[half],
        )

    def r2copy(q, half):
        return rcopy(
            cb.at[q, 1 + half, :, wide(q)], gg.at[q, half, :, wide(q)], q, 3 + half, to_y[half],
        )

    def both(q, yy):
        w = CWP[CHUNKS[q][0]]
        return pp[q, yy, core, :, 0:w].astype(F32) + dd[q, yy, :, 0:w].astype(F32)

    @step
    def _pj(q):
        col, j = CHUNKS[q]
        if j == 3:
            for k in range(4):
                for i in range(2):
                    ocopy(col, JF[k], 2, 1 + i, 12 + 2 * k + i, 0, 1).wait_recv()
        n = CW[col]
        wref = (oa, ob)[col]
        rows = pl.ds(pl.multiple_of(at_s(q) * n, 16), n)

        def part(i, carry):
            tok = pl.ds(pl.multiple_of(i * 256, 256), 256)
            o = None
            for h in range(2):
                d = lax.dot_general(
                    att[h, tok, :], wref[rows, h * 256:(h + 1) * 256],
                    (((1,), (1,)), ((), ())), preferred_element_type=F32,
                )
                o = d if o is None else o + d
            o = o.astype(BF)
            for g in range(4):
                pp[q, i * 2 + g // 2, g % 2, :, 0:n] = o[g * SUB:(g + 1) * SUB]
            return carry

        lax.fori_loop(0, 2, part, 0)
        r0copy(q).start()

    @step
    def _r1(q):
        w = CWP[CHUNKS[q][0]]
        r0copy(q).wait_recv()
        cb[q, 0, :, 0:w] = both(q, yo).astype(BF)
        r1copy(q, 0).start()
        r1copy(q, 1).start()

    @step
    def _r2(q, i):
        w = CWP[CHUNKS[q][0]]
        r1copy(q, i).wait_recv()
        a = both(q, (yp, ym)[i])
        add = slice(32 * i, 32 * i + 32)
        rest = slice(32 - 32 * i, 64 - 32 * i)
        cb[q, 1 + i, add, 0:w] = (a[add] + ee[q, i, :, 0:w].astype(F32)).astype(BF)
        cb[q, 1 + i, rest, 0:w] = a[rest].astype(BF)
        r2copy(q, i).start()

    @step
    def _r3(q):
        w = CWP[CHUNKS[q][0]]
        r2copy(q, 0).wait_recv()
        r2copy(q, 1).wait_recv()
        v = both(q, y) + gg[q, 0, :, 0:w].astype(F32) + gg[q, 1, :, 0:w].astype(F32)
        (sa, sb)[CHUNKS[q][0]][at_s(q)] = v

    @step
    def _zero():
        for q in range(8):
            if CHUNKS[q][0] == 0:
                for g in range(8):
                    pp[q, g // 2, g % 2, :, 512:640] = jnp.zeros((SUB, 128), BF)

    for line in ORDER:
        name, *nums = line.split(",")
        steps[name](*[int(v) for v in nums])

    for i in range(16):
        zi, xi = i // 4, i % 4
        full[:, i * BLK:i * BLK + ON[0]] = sa[zi, :, xi * ON[0]:(xi + 1) * ON[0]]
        full[:, i * BLK + ON[0]:(i + 1) * BLK] = sb[xi, :, zi * ON[1]:(zi + 1) * ON[1]]

    def final(i, carry):
        rows = pl.ds(pl.multiple_of(i * 16, 16), 16)
        v = full[rows, :]
        r = lax.rsqrt(jnp.mean(v * v, axis=-1, keepdims=True) + EPSILON)
        out_v[rows, :] = (hid[rows, :].astype(F32) + v * r * post[...]).astype(BF)
        return carry

    lax.fori_loop(0, SUB // 16, final, 0)

    for p in range(2):
        remote(ws[p], ws[p], wsend.at[p], wrecv.at[p, 0], to_pt).wait_send()
    for col in range(2):
        ref = (oa, ob)[col].at[pl.ds(0, 15 * ON[col]), :]
        remote(ref, ref, osend.at[col], orecv.at[col, 0], to_pt).wait_send()
    ref = xs.at[pl.ds(0, 15 * SUB), :]
    remote(ref, ref, xsend, xrecv.at[0], to_pt).wait_send()
    for half in range(2):

        @pl.when(c < 14)
        def _():
            for i in range(2):
                kcopy(half, i).wait_send()

        for i in range(2):

            @pl.when((cq, cn)[i] < 14)
            def _():
                kfinal(half, i, b, to_xq).wait_send()

    for i in range(4):
        swap(i, False).wait_send()
    for q in range(8):
        r0copy(q).wait_send()
        for half in range(2):
            r1copy(q, half).wait_send()
            r2copy(q, half).wait_send()


def local(
    hidden_in, stretch_start, pre_gain, q_weight, k_weight, v_weight, o_weight, q_gain, k_gain,
    prior_keys, prior_values, post_gain,
):
    frequency = 10000.0 ** (-jnp.arange(HD // 2, dtype=F32) / (HD // 2))
    freq2 = jnp.concatenate([frequency, frequency]).reshape(1, HD)
    hbm = pl.BlockSpec(memory_space=pl.ANY)
    vm = pl.BlockSpec(memory_space=pltpu.VMEM)
    sm = pl.BlockSpec(memory_space=pltpu.SMEM)
    dma = pltpu.SemaphoreType.DMA
    return pl.pallas_call(
        body,
        out_shape=jax.ShapeDtypeStruct((SUB, D), BF),
        in_specs=[hbm, sm, hbm, hbm, hbm, hbm, hbm, vm, vm, hbm, hbm, hbm, vm],
        out_specs=vm,
        scratch_shapes=[
            pltpu.VMEM((D, 256), BF), pltpu.VMEM((D, 256), BF),
            pltpu.VMEM((16 * ON[0], 512), BF), pltpu.VMEM((16 * ON[1], 512), BF),
            pltpu.VMEM((2, 2, BLK, 256), BF), pltpu.VMEM((2, 2, 176, 256), BF),
            pltpu.VMEM((PAIR, D), BF),
            pltpu.VMEM((2, WINDOW + PAIR, HD), BF), pltpu.VMEM((2, 2, TOK, HD), BF),
            pltpu.VMEM((2, PAIR, HD), BF),
            pltpu.VMEM((2, TOK, 256), BF), pltpu.VMEM((TOK, 256), BF),
            pltpu.VMEM((TOK, 256), F32),
            pltpu.VMEM((SUB, D), BF), pltpu.VMEM((1, D), F32), pltpu.VMEM((1, D), F32),
            pltpu.VMEM((PAIR, HD), F32), pltpu.VMEM((PAIR, HD), F32),
            pltpu.VMEM((8, 4, 2, SUB, 768), BF),
            pltpu.VMEM((8, 4, SUB, 768), BF),
            pltpu.VMEM((8, 2, SUB // 2, 768), BF),
            pltpu.VMEM((8, 2, SUB, 768), BF),
            pltpu.VMEM((8, 3, SUB, 768), BF),
            pltpu.VMEM((4, SUB, CWP[0]), F32), pltpu.VMEM((4, SUB, CWP[1]), F32),
            pltpu.VMEM((SUB, D), F32),
            dma((16,)), dma((2,)), dma((2, 22)), dma((2,)), dma((2, 20)), dma, dma((24,)),
            dma((2, 2)), dma((2, 2)), dma((2, 2)), dma((2, 2)), dma((4,)), dma((4,)),
            dma((8, 5)), dma((8, 5)),
        ],
        compiler_params=pltpu.CompilerParams(
            collective_id=0, has_side_effects=True, vmem_limit_bytes=64 * 1024 * 1024 - 128 * 1024
        ),
        name="layer",
    )(
        hidden_in, stretch_start, pre_gain, q_weight, k_weight, v_weight,
        o_weight.T, q_gain.reshape(1, HD), k_gain.reshape(1, HD), prior_keys, prior_values,
        post_gain, freq2,
    )


def solution(mesh):
    return jax.shard_map(
        local,
        mesh=mesh,
        in_specs=(
            P(("ctx", "tp"), None), P(), P(), P("ctx", "tp"), P("ctx", "tp"), P("ctx", "tp"),
            P("tp", "ctx"), P(), P(), P(None, "tp"), P(None, "tp"), P(),
        ),
        out_specs=P(("ctx", "tp"), None),
        check_vma=False,
    )
```

```python
import jax
import jax.numpy as jnp
from jax import lax
from jax.experimental import pallas as pl
from jax.experimental.pallas import tpu as pltpu
from jax.sharding import PartitionSpec as P

HD = 128
WINDOW = 1024
EPSILON = 1e-06
QUERY_FACTOR = 168.0 ** (-0.5)
MESH = pl.DeviceIdType.MESH

D = 5376
BLK = 336
TOK = 512
PAIR = 1024
SUB = 64
HALF = (0, 336), (0, 176), (176, 160)
ON = (192, 144)
OX = ((0, 0), (0, 192)), ((0, 0), (0, 144))
OZ = ((0, 96), (96, 96)), ((0, 80), (80, 64))
CW = (768, 576)
CWP = (768, 640)
KT = 2688
QT = 2688
BF = jnp.bfloat16
F32 = jnp.float32


def body(
    hid_h, start_s, pre_h, q_h, k_h, v_h, o_h, qg_v, kg_v, pk_h, pv_h, post_h, freq_v,
    out_v,
    w0, w1, oa, ob, ow, rb, xs, kv, kr, qb, att, ast, acc, accq, hid, pre, post, cos, sin,
    pp, dd, ee, gg, cb, sa, sb, full,
    lsem, wsend, wrecv, osend, orecv, xsend, xrecv, krsend, krrecv, kfsend, kfrecv,
    swsend, swrecv, rsend, rrecv,
):
    c = lax.axis_index("ctx")
    t = lax.axis_index("tp")
    z, x = c // 4, c % 4
    y, core = t // 2, t % 2
    b = x % 2
    nb = 1 - b
    ws = (w0, w1)

    def nxt(a, d):
        return (a + d + 4) % 4

    def pairx(xx):
        return xx + 1 - 2 * (xx % 2)

    def otherx(xx):
        return (xx + 3 + 2 * (xx % 2)) % 4

    xq, xn, xo = pairx(x), otherx(x), nxt(x, 2)
    yp, ym, yo = nxt(y, 1), nxt(y, -1), nxt(y, 2)
    other = 1 - core
    to_yp = {"ctx": c, "tp": yp * 2 + core}
    to_ym = {"ctx": c, "tp": ym * 2 + core}
    to_pt = {"ctx": c, "tp": y * 2 + other}

    def dev(ci):
        return {"ctx": ci, "tp": t}

    to_xq, to_xn = dev(z * 4 + xq), dev(z * 4 + xn)
    to_zp, to_zm = dev(nxt(z, 1) * 4 + x), dev(nxt(z, -1) * 4 + x)

    def remote(src, dst, ssem, rsem, to):
        return pltpu.make_async_remote_copy(
            src_ref=src, dst_ref=dst, send_sem=ssem, recv_sem=rsem, device_id=to,
            device_id_type=MESH,
        )

    cq, cn = z * 4 + xq, z * 4 + xn
    behind = (c + 14) % 16
    zb, xb = behind // 4, behind % 4
    barrier = pltpu.get_barrier_semaphore()
    peers = [to_yp, to_ym, to_pt, to_xq, to_xn, to_zp, to_zm]
    peers += [dev((cq + 2) % 16), dev((cn + 2) % 16)]
    peers += [dev(zb * 4 + pairx(xb)), dev(zb * 4 + otherx(xb))]
    for peer in peers:
        pl.semaphore_signal(barrier, inc=1, device_id=peer, device_id_type=MESH)

    own = pl.ds(pl.multiple_of(c * BLK, 16), BLK)
    hc = pl.ds(pl.multiple_of(b * HD, HD), HD)
    lo, hi = pl.ds(0, HD), pl.ds(HD, HD)
    loads0 = [
        pltpu.make_async_copy(k_h.at[:, lo], ow.at[0, 0, :, lo], lsem.at[0]),
        pltpu.make_async_copy(v_h.at[:, lo], ow.at[0, 0, :, hi], lsem.at[1]),
        pltpu.make_async_copy(k_h.at[:, hi], ow.at[0, 1, :, lo], lsem.at[2]),
        pltpu.make_async_copy(v_h.at[:, hi], ow.at[0, 1, :, hi], lsem.at[3]),
        pltpu.make_async_copy(k_h.at[:, hc], w0.at[own, lo], lsem.at[4]),
        pltpu.make_async_copy(v_h.at[:, hc], w0.at[own, hi], lsem.at[5]),
    ]
    loadx = [
        pltpu.make_async_copy(hid_h, hid, lsem.at[6]),
        pltpu.make_async_copy(pre_h, pre.at[0], lsem.at[7]),
    ]
    loads1 = [
        pltpu.make_async_copy(q_h.at[:, pl.ds(0, 256)], ow.at[1, 0], lsem.at[8]),
        pltpu.make_async_copy(q_h.at[:, pl.ds(256, 256)], ow.at[1, 1], lsem.at[9]),
        pltpu.make_async_copy(
            q_h.at[:, pl.ds(pl.multiple_of(b * 256, 256), 256)], w1.at[own, :], lsem.at[10]
        ),
    ]
    loads2 = [
        pltpu.make_async_copy(
            o_h.at[pl.ds(0, ON[0]), :],
            oa.at[pl.ds(pl.multiple_of(c * ON[0], 16), ON[0]), :], lsem.at[11],
        ),
        pltpu.make_async_copy(
            o_h.at[pl.ds(ON[0], ON[1]), :],
            ob.at[pl.ds(pl.multiple_of((x * 4 + z) * ON[1], 16), ON[1]), :], lsem.at[12],
        ),
        pltpu.make_async_copy(post_h, post.at[0], lsem.at[13]),
    ]
    for load in loadx + loads0 + loads1 + loads2:
        load.start()

    def prior(i):
        return pltpu.make_async_copy(
            (pk_h, pv_h)[i].at[:, hc], kv.at[i, pl.ds(0, WINDOW), :], lsem.at[14 + i]
        )

    @pl.when(c < 2)
    def _():
        prior(0).start()
        prior(1).start()

    for load in loadx:
        load.wait()

    def prenorm(i, carry):
        rows = pl.ds(pl.multiple_of(i * 16, 16), 16)
        h = hid[rows, :].astype(F32)
        r = lax.rsqrt(jnp.mean(h * h, axis=-1, keepdims=True) + EPSILON)
        to = pl.ds(pl.multiple_of(b * TOK + t * SUB + i * 16, 16), 16)
        xs[to, :] = (h * r * pre[...]).astype(BF)
        return carry

    lax.fori_loop(0, SUB // 16, prenorm, 0)
    pl.semaphore_wait(barrier, len(peers))

    waited = set()

    def need(name, group):
        if name not in waited:
            waited.add(name)
            for load in group:
                load.wait()

    def need_w(p):
        need(p, (loads0, loads1)[p])

    XJ = (x, xq, xn, xo)
    to_z = (to_zp, to_zm)

    def wrows(zz, xx, part):
        off, num = HALF[part]
        return pl.ds(pl.multiple_of((zz * 4 + xx) * BLK + off, 16), num)

    def wx(p, src, xx, part, sem, to):
        return remote(
            src, ws[p].at[wrows(z, xx, part), :], wsend.at[p], wrecv.at[p, sem], to
        )

    def wz(p, zz, j, part, sem, to):
        ref = ws[p].at[wrows(zz, XJ[j], part), :]
        return remote(ref, ref, wsend.at[p], wrecv.at[p, sem], to)

    def relay_in(p, side):
        off, num = HALF[1 + side]
        return remote(
            ow.at[p, b, pl.ds(off, num), :], rb.at[p, side, pl.ds(0, num), :],
            wsend.at[p], wrecv.at[p, 2 + side], (to_xq, to_xn)[side],
        )

    def relay_out(p, side, xx):
        src = rb.at[p, side, pl.ds(0, HALF[1 + side][1]), :]
        return wx(p, src, xx, 1 + side, 4 + side, (to_xn, to_xq)[side])

    def whole(p, side, xx):
        return wx(p, ow.at[p, nb], xx, 0, side, (to_xq, to_xn)[side])

    def wz_out(p, j):
        for i in range(2):
            wz(p, z, j, 0, 6 + 2 * j + i, to_z[i]).start()

    def _wr(p):
        need_w(p)
        relay_in(p, 0).start()
        relay_in(p, 1).start()

    def _ww(p):
        need_w(p)
        whole(p, 0, x).start()
        whole(p, 1, x).start()

    def _wz0(p):
        need_w(p)
        wz_out(p, 0)

    def _wf(p, side):
        relay_in(p, side).wait_recv()
        relay_out(p, side, (xq, xn)[side]).start()

    def _wzx(p, j):
        whole(p, j - 1, XJ[j]).wait_recv()
        wz_out(p, j)

    def _wzo(p):
        relay_out(p, 0, xo).wait_recv()
        relay_out(p, 1, xo).wait_recv()
        wz_out(p, 3)

    def _wfw(p, j, i):
        zz = nxt(z, (-1, 1)[i])
        wz(p, zz, j, 0, 6 + 2 * j + i, to_z[i]).wait_recv()
        wz(p, zz, j, 1 + i, 14 + 2 * j + i, to_z[i]).start()

    def _wl(p):
        for j in range(4):
            for i in range(2):
                wz(p, nxt(z, 2), j, 1 + i, 14 + 2 * j + i, to_z[i]).wait_recv()

    AX = ((xq, xn), (xq, xn), (1, 0), xo, OX)
    AZ = ((nxt(z, 1), nxt(z, -1)), (nxt(z, -1), nxt(z, 1)), (0, 1), nxt(z, 2), OZ)
    AXES = ((AX, AZ), (AZ, AX))
    HERE = ((x, z), (z, x))

    def first_of(col, j):
        axis = AXES[col][0]
        return (HERE[col][0], axis[1][0], axis[1][1], axis[3])[j]

    def ocopy(col, f, s, part, sem, to_f, to_s):
        off, num = (0, ON[col]) if part is None else part
        row = (s * 4 + f) * ON[col] + off
        ref = (oa, ob)[col].at[pl.ds(pl.multiple_of(row, 16), num), :]
        to = dev(to_s * 4 + to_f if col == 0 else to_f * 4 + to_s)
        return remote(ref, ref, osend.at[col], orecv.at[col, sem], to)

    def _o0(col, i):
        need(2, loads2)
        f, s = HERE[col]
        ocopy(col, f, s, None, i, AXES[col][0][0][i], s).start()

    def _o1(col, i):
        send, recv, way, _, parts = AXES[col][0]
        s, w = HERE[col][1], way[i]
        ocopy(col, recv[i], s, None, i, send[i], s).wait_recv()
        if parts[col][w][1]:
            ocopy(col, recv[i], s, parts[col][w], 2 + w, send[w], s).start()

    def _o3(col):
        send, _, _, far, parts = AXES[col][0]
        s = HERE[col][1]
        for w in range(2):
            if parts[col][w][1]:
                ocopy(col, far, s, parts[col][w], 2 + w, send[w], s).wait_recv()

    def _os(col, j, i):
        need(2, loads2)
        f, s = HERE[col]
        ocopy(col, first_of(col, j), s, None, 4 + 2 * j + i, f, AXES[col][1][0][i]).start()

    def _of(col, j, i):
        send, recv, way, _, parts = AXES[col][1]
        f, w = HERE[col][0], way[i]
        fj = first_of(col, j)
        ocopy(col, fj, recv[i], None, 4 + 2 * j + i, f, send[i]).wait_recv()
        if parts[col][w][1]:
            ocopy(col, fj, recv[i], parts[col][w], 12 + 2 * j + w, f, send[w]).start()

    def ofar(col):
        send, _, _, far, parts = AXES[col][1]
        f = HERE[col][0]
        for j in range(4):
            for w in range(2):
                if parts[col][w][1]:
                    ocopy(
                        col, first_of(col, j), far, parts[col][w], 12 + 2 * j + w, f, send[w]
                    ).wait_recv()

    CC = (b, nb)

    def xcopy(cc, yy, kk, part, sem, to):
        off, num = ((0, SUB), (0, SUB // 2), (SUB // 2, SUB // 2))[part]
        row = CC[cc] * TOK + (yy * 2 + kk) * SUB + off
        ref = xs.at[pl.ds(pl.multiple_of(row, 16), num), :]
        return remote(ref, ref, xsend, xrecv.at[sem], to)

    to_y = (to_yp, to_ym)

    def xsem(cc, k):
        return cc * 12 + k

    def _xp(h):
        xcopy(0, y, core, 1 + h, 24 + h, to_xq).start()

    def xout(cc, h):
        for i in range(2):
            xcopy(cc, y, core, 1 + h, xsem(cc, 2 * i + h), to_y[i]).start()
        xcopy(cc, y, core, 1 + h, xsem(cc, 6 + h), to_pt).start()

    def _xo(h):
        xout(0, h)

    def _xg(h):
        xcopy(1, y, core, 1 + h, 24 + h, to_xq).wait_recv()
        xout(1, h)

    YB = (ym, yp)

    def _xf(cc, i):
        xcopy(cc, YB[i], core, 1 + i, xsem(cc, 3 * i), to_y[i]).wait_recv()
        xcopy(cc, YB[i], core, 1 + i, xsem(cc, 4 + i), to_y[i]).start()

    def _xm(cc, i):
        xcopy(cc, YB[i], core, 2 - i, xsem(cc, 1 + i), to_y[i]).wait_recv()
        xcopy(cc, YB[i], core, 0, xsem(cc, 8 + i), to_pt).start()

    def _xt(cc, i):
        xcopy(cc, yo, core, 1 + i, xsem(cc, 4 + i), to_y[i]).wait_recv()
        xcopy(cc, yo, core, 1 + i, xsem(cc, 10 + i), to_pt).start()

    def _xd(g):
        cc = (0, 1, 1)[g]
        if g < 2:
            xcopy(cc, y, other, 1, xsem(cc, 6), to_pt).wait_recv()
            xcopy(cc, y, other, 2, xsem(cc, 7), to_pt).wait_recv()
            xcopy(cc, ym, other, 0, xsem(cc, 8), to_pt).wait_recv()
            xcopy(cc, yp, other, 0, xsem(cc, 9), to_pt).wait_recv()
        if g != 1:
            xcopy(cc, yo, other, 1, xsem(cc, 10), to_pt).wait_recv()
            xcopy(cc, yo, other, 2, xsem(cc, 11), to_pt).wait_recv()

    base = WINDOW + (c - b) * TOK

    def _ang():
        def angle(i, carry):
            rows = pl.ds(pl.multiple_of(i * 128, 128), 128)
            pos = lax.broadcasted_iota(jnp.int32, (128, HD), 0) + (base + i * 128)
            a = pos.astype(F32) * freq_v[...]
            lane = lax.broadcasted_iota(jnp.int32, (128, HD), 1)
            cos[rows, :] = jnp.cos(a)
            sn = jnp.sin(a)
            sin[rows, :] = jnp.where(lane < HD // 2, -sn, sn)
            return carry

        lax.fori_loop(0, PAIR // 128, angle, 0)

    BLOCKS = (None, (y, ym, yp), (yo,))

    def tokens(g, i):
        return CC[0] * TOK + i * 128 if g == 0 else CC[1] * TOK + BLOCKS[g][i] * 128

    def at(start):
        return pl.ds(pl.multiple_of(start, 128), 128)

    def mm(w, g, out, k0, kt, steps, fresh):
        num = (TOK, 384, 128)[g]

        def part(i, carry):
            ks = pl.ds(pl.multiple_of(k0 + i * kt, 128), kt)
            if g == 0:
                rows = xs[pl.ds(pl.multiple_of(CC[0] * TOK, TOK), TOK), ks]
            else:
                rows = [xs[at(tokens(g, k)), ks] for k in range(num // 128)]
                rows = jnp.concatenate(rows, axis=0) if num > 128 else rows[0]
            out[...] += jnp.dot(rows, w[ks, :], preferred_element_type=F32)
            return carry

        if fresh:
            out[...] = jnp.zeros((num, 256), F32)
        lax.fori_loop(0, steps, part, 0)

    def each(g, fn):
        if g == 0:

            def go(i, carry):
                fn(pl.multiple_of(i * 128, 128), tokens(0, i))
                return carry

            lax.fori_loop(0, 4, go, 0)
        else:
            for i in range((0, 3, 1)[g]):
                fn(i * 128, tokens(g, i))

    def headed(raw, tok, gain):
        r = lax.rsqrt(jnp.mean(raw * raw, axis=-1, keepdims=True) + EPSILON)
        n = raw * r * gain[...]
        return n * cos[at(tok), :] + pltpu.roll(n, HD // 2, 1) * sin[at(tok), :]

    def krows(m, cc):
        if m == 0:
            return 0, CC[cc] * TOK, TOK
        blk = (y, ym, yp, yo)[m - 1]
        return blk * 128, CC[1 - cc] * TOK + blk * 128, 128

    def kcopy(m, i):
        slot, row, num = krows(m, 0)
        return remote(
            kv.at[i, pl.ds(pl.multiple_of(WINDOW + row, 128), num), :],
            kr.at[0 if m == 0 else 1, i, pl.ds(pl.multiple_of(slot, 128), num), :],
            krsend.at[i, m], krrecv.at[i, m], (to_xq, to_xn)[i],
        )

    def kfinal(m, i, cc, to):
        slot, row, num = krows(m, cc)
        return remote(
            kr.at[0 if m == 0 else 1, i, pl.ds(pl.multiple_of(slot, 128), num), :],
            kv.at[i, pl.ds(pl.multiple_of(row, 128), num), :],
            kfsend.at[i, m], kfrecv.at[i, m], to,
        )

    def _mk(g):
        mm(w0, g, acc.at[pl.ds(0, (TOK, 384, 128)[g]), :], 0, KT, D // KT, True)

        def keys(row, tok):
            raw = acc[pl.ds(row, 128), 0:HD]
            kv[0, at(WINDOW + tok), :] = headed(raw, tok, kg_v).astype(BF)
            kv[1, at(WINDOW + tok), :] = acc[pl.ds(row, 128), HD:2 * HD].astype(BF)

        each(g, keys)

        @pl.when(c < 14)
        def _():
            for m in ((0,), (1, 2, 3), (4,))[g]:
                for i in range(2):
                    kcopy(m, i).start()

    def _kvf(m, i):
        src = (cq, cn)[i]

        @pl.when(src < 14)
        def _():
            kcopy(m, i).wait_recv()
            kfinal(m, i, 1, dev((src + 2) % 16)).start()

    def qhalf(g, second):
        start = (0, TOK, TOK + 384)[g]
        out = accq.at[pl.ds(start, (TOK, 384, 128)[g]), :]
        z2 = 1 - z // 2 if second else z // 2
        mm(w1, g, out, z2 * (D // 2), QT, D // 2 // QT, not second)

    def _mqa(g):
        qhalf(g, False)

    def _mqb(g):
        qhalf(g, True)

        def queries(row, tok):
            for h in range(2):
                raw = accq[pl.ds((0, TOK, TOK + 384)[g] + row, 128), h * HD:(h + 1) * HD]
                qb[h, at(tok), :] = (headed(raw, tok, qg_v) * QUERY_FACTOR).astype(BF)

        each(g, queries)

    def _aw():
        @pl.when(c < 2)
        def _():
            prior(0).wait()
            prior(1).wait()

        @pl.when(c >= 2)
        def _():
            for m in range(5):
                for i in range(2):
                    kfinal(m, i, 0, to_xq).wait_recv()

    first = WINDOW - start_s[0] - (c - b) * TOK

    def attend(q0):
        q = qb[:, pl.ds(q0, 128), :].reshape(256, HD)
        k = kv[0, pl.ds(q0, 1152), :]
        v = kv[1, pl.ds(q0, 1152), :]
        s = lax.dot_general(q, k, (((1,), (1,)), ((), ())), preferred_element_type=F32)
        j = lax.broadcasted_iota(jnp.int32, (256, 1152), 1)
        r = lax.broadcasted_iota(jnp.int32, (256, 1152), 0)
        r = jnp.where(r >= 128, r - 128, r)
        s = jnp.where((j > r) & (j <= r + WINDOW) & (j >= first - q0), s, F32(-1e30))
        m = jnp.max(s, axis=-1, keepdims=True)
        e = jnp.exp(s - m)
        total = jnp.sum(e, axis=-1, keepdims=True)
        return (jnp.dot(e.astype(BF), v, preferred_element_type=F32) / total).astype(BF)

    def swap(i, from_pair):
        rows = pl.ds(i * 128, 128)
        half = nb if from_pair else b
        return remote(ast.at[rows, :], att.at[half, rows, :], swsend.at[i], swrecv.at[i], to_xq)

    def _au(i):
        o = attend(pl.multiple_of(nb * TOK + i * 128, 128))
        ast[i * 128:(i + 1) * 128, 0:128] = o[:128]
        ast[i * 128:(i + 1) * 128, 128:256] = o[128:]
        swap(i, False).start()

    def _ao(i):
        o = attend(pl.multiple_of(b * TOK + i * 128, 128))
        att[b, i * 128:(i + 1) * 128, 0:128] = o[:128]
        att[b, i * 128:(i + 1) * 128, 128:256] = o[128:]

    def _sw():
        for i in range(4):
            swap(i, True).wait_recv()

    CHUNKS = [(0, 0), (1, 0), (0, 1), (0, 2), (1, 1), (1, 2), (0, 3), (1, 3)]

    def at_s(q):
        col, j = CHUNKS[q]
        axis = AXES[col][1]
        return (HERE[col][1], axis[1][0], axis[1][1], axis[3])[j]

    def wide(q):
        return pl.ds(0, CWP[CHUNKS[q][0]])

    def rcopy(src, dst, q, sem, to):
        return remote(src, dst, rsend.at[q, sem], rrecv.at[q, sem], to)

    def r0copy(q):
        return rcopy(pp.at[q, :, other, :, wide(q)], dd.at[q, :, :, wide(q)], q, 0, to_pt)

    def r1copy(q, half):
        return rcopy(
            cb.at[q, 0, pl.ds(half * 32, 32), wide(q)], ee.at[q, half, :, wide(q)], q, 1 + half,
            to_y[half],
        )

    def r2copy(q, half):
        return rcopy(
            cb.at[q, 1 + half, :, wide(q)], gg.at[q, half, :, wide(q)], q, 3 + half, to_y[half],
        )

    def both(q, yy):
        w = CWP[CHUNKS[q][0]]
        return pp[q, yy, core, :, 0:w].astype(F32) + dd[q, yy, :, 0:w].astype(F32)

    def _pj(q):
        col, j = CHUNKS[q]
        if j == 3:
            ofar(col)
        n = CW[col]
        wref = (oa, ob)[col]
        rows = pl.ds(pl.multiple_of(at_s(q) * n, 16), n)

        def part(i, carry):
            tok = pl.ds(pl.multiple_of(i * 256, 256), 256)
            o = None
            for h in range(2):
                d = lax.dot_general(
                    att[h, tok, :], wref[rows, h * 256:(h + 1) * 256],
                    (((1,), (1,)), ((), ())), preferred_element_type=F32,
                )
                o = d if o is None else o + d
            o = o.astype(BF)
            for g in range(4):
                pp[q, i * 2 + g // 2, g % 2, :, 0:n] = o[g * SUB:(g + 1) * SUB]
            return carry

        lax.fori_loop(0, 2, part, 0)
        r0copy(q).start()

    def _r1(q):
        w = CWP[CHUNKS[q][0]]
        r0copy(q).wait_recv()
        cb[q, 0, :, 0:w] = both(q, yo).astype(BF)
        r1copy(q, 0).start()
        r1copy(q, 1).start()

    def _r2(q, i):
        w = CWP[CHUNKS[q][0]]
        r1copy(q, i).wait_recv()
        a = both(q, (yp, ym)[i])
        add = slice(32 * i, 32 * i + 32)
        rest = slice(32 - 32 * i, 64 - 32 * i)
        cb[q, 1 + i, add, 0:w] = (a[add] + ee[q, i, :, 0:w].astype(F32)).astype(BF)
        cb[q, 1 + i, rest, 0:w] = a[rest].astype(BF)
        r2copy(q, i).start()

    def _r3(q):
        w = CWP[CHUNKS[q][0]]
        r2copy(q, 0).wait_recv()
        r2copy(q, 1).wait_recv()
        v = both(q, y) + gg[q, 0, :, 0:w].astype(F32) + gg[q, 1, :, 0:w].astype(F32)
        (sa, sb)[CHUNKS[q][0]][at_s(q)] = v

    def _zero():
        for q in range(8):
            if CHUNKS[q][0] == 1:
                for g in range(8):
                    pp[q, g // 2, g % 2, :, 512:640] = jnp.zeros((SUB, 128), BF)

    for fn, *nums in (
        (_xo, 1), (_ww, 0), (_xp, 1), (_wz0, 1), (_o0, 1, 1), (_o0, 1, 0), (_xo, 0),
        (_wfw, 1, 0, 1), (_o0, 0, 1), (_wz0, 0), (_wzx, 0, 1), (_wzx, 0, 2), (_xp, 0),
        (_wr, 0), (_o1, 0, 1), (_wf, 0, 1), (_xg, 1), (_wfw, 1, 0, 0), (_o1, 1, 1),
        (_o1, 1, 0), (_o0, 0, 0), (_ww, 1), (_wzx, 1, 2), (_wr, 1), (_xg, 0), (_xf, 0, 0),
        (_wf, 0, 0), (_wfw, 0, 2, 1), (_os, 1, 1, 1), (_wfw, 0, 0, 0), (_wf, 1, 1), (_wzo, 0),
        (_xf, 0, 1), (_os, 1, 0, 0), (_wfw, 0, 0, 1), (_wfw, 0, 1, 0), (_os, 1, 2, 1),
        (_xf, 1, 1), (_os, 1, 2, 0), (_o1, 0, 0), (_wfw, 0, 1, 1), (_xm, 0, 0),
        (_of, 1, 1, 1), (_ang,), (_zero,), (_wfw, 0, 2, 0), (_o3, 1), (_wfw, 0, 3, 1),
        (_xm, 1, 1), (_wf, 1, 0), (_xf, 1, 0), (_xm, 0, 1), (_wfw, 0, 3, 0), (_xm, 1, 0),
        (_wzx, 1, 1), (_os, 1, 3, 1), (_wzo, 1), (_xd, 1), (_wl, 0), (_wfw, 1, 2, 1),
        (_xt, 0, 1), (_xt, 0, 0), (_mk, 1), (_wfw, 1, 1, 1), (_xd, 0), (_mk, 0),
        (_wfw, 1, 2, 0), (_kvf, 3, 1), (_xt, 1, 0), (_wfw, 1, 3, 0), (_of, 1, 2, 1),
        (_wfw, 1, 3, 1), (_kvf, 1, 0), (_kvf, 3, 0), (_kvf, 2, 1), (_kvf, 2, 0),
        (_wfw, 1, 1, 0), (_os, 0, 0, 0), (_kvf, 1, 1), (_xt, 1, 1), (_os, 0, 2, 1), (_xd, 2),
        (_mk, 2), (_kvf, 0, 1), (_kvf, 0, 0), (_o3, 0), (_mqa, 0), (_mqa, 1), (_os, 0, 3, 0),
        (_mqa, 2), (_os, 0, 3, 1), (_os, 0, 0, 1), (_kvf, 4, 1), (_kvf, 4, 0), (_wl, 1),
        (_mqb, 1), (_of, 1, 3, 1), (_mqb, 2), (_os, 0, 1, 0), (_os, 0, 1, 1), (_of, 0, 2, 1),
        (_os, 0, 2, 0), (_os, 1, 0, 1), (_aw,), (_au, 0), (_au, 1), (_au, 2), (_au, 3),
        (_os, 1, 3, 0), (_mqb, 0), (_ao, 0), (_ao, 1), (_ao, 2), (_ao, 3), (_sw,), (_pj, 1),
        (_os, 1, 1, 0), (_of, 0, 3, 0), (_of, 1, 2, 0), (_of, 1, 0, 1), (_pj, 0), (_r1, 1),
        (_pj, 5), (_r1, 0), (_of, 1, 3, 0), (_of, 0, 1, 0), (_r1, 5), (_of, 1, 0, 0),
        (_r2, 1, 1), (_r2, 1, 0), (_of, 0, 1, 1), (_of, 0, 0, 0), (_r2, 0, 0), (_r2, 0, 1),
        (_of, 0, 2, 0), (_of, 0, 3, 1), (_pj, 2), (_of, 1, 1, 0), (_pj, 4), (_r1, 2),
        (_r2, 5, 0), (_of, 0, 0, 1), (_r1, 4), (_pj, 3), (_r2, 5, 1), (_r1, 3), (_r2, 2, 0),
        (_r2, 2, 1), (_r2, 4, 1), (_r3, 0), (_pj, 7), (_r2, 4, 0), (_pj, 6), (_r1, 7),
        (_r1, 6), (_r2, 3, 0), (_r3, 1), (_r2, 3, 1), (_r3, 2), (_r3, 4), (_r2, 7, 1),
        (_r2, 7, 0), (_r2, 6, 1), (_r3, 5), (_r2, 6, 0), (_r3, 3), (_r3, 7), (_r3, 6),
    ):
        fn(*nums)

    for i in range(16):
        zi, xi = i // 4, i % 4
        full[:, i * BLK:i * BLK + ON[0]] = sa[zi, :, xi * ON[0]:(xi + 1) * ON[0]]
        full[:, i * BLK + ON[0]:(i + 1) * BLK] = sb[xi, :, zi * ON[1]:(zi + 1) * ON[1]]

    def final(i, carry):
        rows = pl.ds(pl.multiple_of(i * 16, 16), 16)
        v = full[rows, :]
        r = lax.rsqrt(jnp.mean(v * v, axis=-1, keepdims=True) + EPSILON)
        out_v[rows, :] = (hid[rows, :].astype(F32) + v * r * post[...]).astype(BF)
        return carry

    lax.fori_loop(0, SUB // 16, final, 0)

    for p in range(2):
        remote(ws[p], ws[p], wsend.at[p], wrecv.at[p, 0], to_pt).wait_send()
    for col in range(2):
        ref = (oa, ob)[col].at[pl.ds(0, 15 * ON[col]), :]
        remote(ref, ref, osend.at[col], orecv.at[col, 0], to_pt).wait_send()
    ref = xs.at[pl.ds(0, 15 * SUB), :]
    remote(ref, ref, xsend, xrecv.at[0], to_pt).wait_send()
    for m in range(5):
        for i in range(2):

            @pl.when(c < 14)
            def _():
                kcopy(m, i).wait_send()

            @pl.when((cq, cn)[i] < 14)
            def _():
                kfinal(m, i, 1, to_xq).wait_send()

    for i in range(4):
        swap(i, False).wait_send()
    for q in range(8):
        r0copy(q).wait_send()
        for half in range(2):
            r1copy(q, half).wait_send()
            r2copy(q, half).wait_send()


def local(
    hidden_in, stretch_start, pre_gain, q_weight, k_weight, v_weight, o_weight, q_gain, k_gain,
    prior_keys, prior_values, post_gain,
):
    frequency = 10000.0 ** (-jnp.arange(HD // 2, dtype=F32) / (HD // 2))
    freq2 = jnp.concatenate([frequency, frequency]).reshape(1, HD)
    hbm = pl.BlockSpec(memory_space=pl.ANY)
    vm = pl.BlockSpec(memory_space=pltpu.VMEM)
    sm = pl.BlockSpec(memory_space=pltpu.SMEM)
    dma = pltpu.SemaphoreType.DMA
    return pl.pallas_call(
        body,
        out_shape=jax.ShapeDtypeStruct((SUB, D), BF),
        in_specs=[hbm, sm, hbm, hbm, hbm, hbm, hbm, vm, vm, hbm, hbm, hbm, vm],
        out_specs=vm,
        scratch_shapes=[
            pltpu.VMEM((D, 256), BF), pltpu.VMEM((D, 256), BF),
            pltpu.VMEM((16 * ON[0], 512), BF), pltpu.VMEM((16 * ON[1], 512), BF),
            pltpu.VMEM((2, 2, BLK, 256), BF), pltpu.VMEM((2, 2, 176, 256), BF),
            pltpu.VMEM((PAIR, D), BF),
            pltpu.VMEM((2, WINDOW + PAIR, HD), BF), pltpu.VMEM((2, 2, TOK, HD), BF),
            pltpu.VMEM((2, PAIR, HD), BF),
            pltpu.VMEM((2, TOK, 256), BF), pltpu.VMEM((TOK, 256), BF),
            pltpu.VMEM((TOK, 256), F32), pltpu.VMEM((PAIR, 256), F32),
            pltpu.VMEM((SUB, D), BF), pltpu.VMEM((1, D), F32), pltpu.VMEM((1, D), F32),
            pltpu.VMEM((PAIR, HD), F32), pltpu.VMEM((PAIR, HD), F32),
            pltpu.VMEM((8, 4, 2, SUB, 768), BF),
            pltpu.VMEM((8, 4, SUB, 768), BF),
            pltpu.VMEM((8, 2, SUB // 2, 768), BF),
            pltpu.VMEM((8, 2, SUB, 768), BF),
            pltpu.VMEM((8, 3, SUB, 768), BF),
            pltpu.VMEM((4, SUB, CWP[0]), F32), pltpu.VMEM((4, SUB, CWP[1]), F32),
            pltpu.VMEM((SUB, D), F32),
            dma((16,)), dma((2,)), dma((2, 22)), dma((2,)), dma((2, 20)), dma, dma((26,)),
            dma((2, 5)), dma((2, 5)), dma((2, 5)), dma((2, 5)), dma((4,)), dma((4,)),
            dma((8, 5)), dma((8, 5)),
        ],
        compiler_params=pltpu.CompilerParams(
            collective_id=0, has_side_effects=True, vmem_limit_bytes=64 * 1024 * 1024 - 128 * 1024
        ),
        name="layer",
    )(
        hidden_in, stretch_start, pre_gain, q_weight, k_weight, v_weight,
        o_weight.T, q_gain.reshape(1, HD), k_gain.reshape(1, HD), prior_keys, prior_values,
        post_gain, freq2,
    )


def solution(mesh):
    return jax.shard_map(
        local,
        mesh=mesh,
        in_specs=(
            P(("ctx", "tp"), None), P(), P(), P("ctx", "tp"), P("ctx", "tp"), P("ctx", "tp"),
            P("tp", "ctx"), P(), P(), P(None, "tp"), P(None, "tp"), P(),
        ),
        out_specs=P(("ctx", "tp"), None),
        check_vma=False,
    )
```

```python
import jax
import jax.numpy as jnp
from jax import lax
from jax.experimental import pallas as pl
from jax.experimental.pallas import tpu as pltpu
from jax.sharding import PartitionSpec as P

HD = 128
WINDOW = 1024
EPSILON = 1e-06
QUERY_FACTOR = 168.0 ** (-0.5)
MESH = pl.DeviceIdType.MESH

D = 5376
BLK = 336
TOK = 512
PAIR = 1024
SUB = 64
HALF = (0, 336), (0, 176), (176, 160)
ON = (192, 144)
OX = ((0, 0), (0, 192)), ((0, 0), (0, 144))
OZ = ((0, 96), (96, 96)), ((0, 80), (80, 64))
CW = (768, 576)
CWP = (768, 640)
KT = 768
BF = jnp.bfloat16
F32 = jnp.float32


def body(
    hid_h, start_s, pre_h, q_h, k_h, v_h, o_h, qg_v, kg_v, pk_h, pv_h, post_h, freq_v,
    out_v,
    w0, w1, oa, ob, ow, rb, xs, kv, kr, qb, att, ast, acc, hid, pre, post, cos, sin,
    pp, dd, ee, gg, cb, sa, sb, full,
    lsem, wsend, wrecv, osend, orecv, xsend, xrecv, krsend, krrecv, kfsend, kfrecv,
    swsend, swrecv, rsend, rrecv,
):
    c = lax.axis_index("ctx")
    t = lax.axis_index("tp")
    z, x = c // 4, c % 4
    y, core = t // 2, t % 2
    b = x % 2
    nb = 1 - b
    ws = (w0, w1)

    def nxt(a, d):
        return (a + d + 4) % 4

    def pairx(xx):
        return xx + 1 - 2 * (xx % 2)

    def otherx(xx):
        return (xx + 3 + 2 * (xx % 2)) % 4

    xq, xn, xo = pairx(x), otherx(x), nxt(x, 2)
    yp, ym, yo = nxt(y, 1), nxt(y, -1), nxt(y, 2)
    other = 1 - core
    to_yp = {"ctx": c, "tp": yp * 2 + core}
    to_ym = {"ctx": c, "tp": ym * 2 + core}
    to_pt = {"ctx": c, "tp": y * 2 + other}

    def dev(ci):
        return {"ctx": ci, "tp": t}

    to_xq, to_xn = dev(z * 4 + xq), dev(z * 4 + xn)
    to_zp, to_zm = dev(nxt(z, 1) * 4 + x), dev(nxt(z, -1) * 4 + x)

    def remote(src, dst, ssem, rsem, to):
        return pltpu.make_async_remote_copy(
            src_ref=src, dst_ref=dst, send_sem=ssem, recv_sem=rsem, device_id=to,
            device_id_type=MESH,
        )

    cq, cn = z * 4 + xq, z * 4 + xn
    behind = (c + 14) % 16
    zb, xb = behind // 4, behind % 4
    barrier = pltpu.get_barrier_semaphore()
    peers = [to_yp, to_ym, to_pt, to_xq, to_xn, to_zp, to_zm]
    peers += [dev((cq + 2) % 16), dev((cn + 2) % 16)]
    peers += [dev(zb * 4 + pairx(xb)), dev(zb * 4 + otherx(xb))]
    for peer in peers:
        pl.semaphore_signal(barrier, inc=1, device_id=peer, device_id_type=MESH)

    own = pl.ds(pl.multiple_of(c * BLK, 16), BLK)
    hc = pl.ds(pl.multiple_of(b * HD, HD), HD)
    lo, hi = pl.ds(0, HD), pl.ds(HD, HD)
    loads0 = [
        pltpu.make_async_copy(k_h.at[:, lo], ow.at[0, 0, :, lo], lsem.at[0]),
        pltpu.make_async_copy(v_h.at[:, lo], ow.at[0, 0, :, hi], lsem.at[1]),
        pltpu.make_async_copy(k_h.at[:, hi], ow.at[0, 1, :, lo], lsem.at[2]),
        pltpu.make_async_copy(v_h.at[:, hi], ow.at[0, 1, :, hi], lsem.at[3]),
        pltpu.make_async_copy(k_h.at[:, hc], w0.at[own, lo], lsem.at[4]),
        pltpu.make_async_copy(v_h.at[:, hc], w0.at[own, hi], lsem.at[5]),
    ]
    loadx = [
        pltpu.make_async_copy(hid_h, hid, lsem.at[6]),
        pltpu.make_async_copy(pre_h, pre.at[0], lsem.at[7]),
    ]
    loads1 = [
        pltpu.make_async_copy(q_h.at[:, pl.ds(0, 256)], ow.at[1, 0], lsem.at[8]),
        pltpu.make_async_copy(q_h.at[:, pl.ds(256, 256)], ow.at[1, 1], lsem.at[9]),
        pltpu.make_async_copy(
            q_h.at[:, pl.ds(pl.multiple_of(b * 256, 256), 256)], w1.at[own, :], lsem.at[10]
        ),
    ]
    loads2 = [
        pltpu.make_async_copy(
            o_h.at[pl.ds(0, ON[0]), :],
            oa.at[pl.ds(pl.multiple_of(c * ON[0], 16), ON[0]), :], lsem.at[11],
        ),
        pltpu.make_async_copy(
            o_h.at[pl.ds(ON[0], ON[1]), :],
            ob.at[pl.ds(pl.multiple_of((x * 4 + z) * ON[1], 16), ON[1]), :], lsem.at[12],
        ),
        pltpu.make_async_copy(post_h, post.at[0], lsem.at[13]),
    ]
    for load in loadx + loads0 + loads1 + loads2:
        load.start()

    def prior(i):
        return pltpu.make_async_copy(
            (pk_h, pv_h)[i].at[:, hc], kv.at[i, pl.ds(0, WINDOW), :], lsem.at[14 + i]
        )

    @pl.when(c < 2)
    def _():
        prior(0).start()
        prior(1).start()

    for load in loadx:
        load.wait()

    def prenorm(i, carry):
        rows = pl.ds(pl.multiple_of(i * 16, 16), 16)
        h = hid[rows, :].astype(F32)
        r = lax.rsqrt(jnp.mean(h * h, axis=-1, keepdims=True) + EPSILON)
        to = pl.ds(pl.multiple_of(b * TOK + t * SUB + i * 16, 16), 16)
        xs[to, :] = (h * r * pre[...]).astype(BF)
        return carry

    lax.fori_loop(0, SUB // 16, prenorm, 0)
    for q in (1, 4, 5, 7):
        for g in range(8):
            pp[q, g // 2, g % 2, :, 512:640] = jnp.zeros((SUB, 128), BF)
    pl.semaphore_wait(barrier, len(peers))

    waited = set()

    def need(name, group):
        if name not in waited:
            waited.add(name)
            for load in group:
                load.wait()

    def need_w(p):
        need(p, (loads0, loads1)[p])

    XJ = (x, xq, xn, xo)
    to_z = (to_zp, to_zm)

    def wrows(zz, xx, part):
        off, num = HALF[part]
        return pl.ds(pl.multiple_of((zz * 4 + xx) * BLK + off, 16), num)

    def wx(p, src, xx, part, sem, to):
        return remote(
            src, ws[p].at[wrows(z, xx, part), :], wsend.at[p], wrecv.at[p, sem], to
        )

    def wz(p, zz, j, part, sem, to):
        ref = ws[p].at[wrows(zz, XJ[j], part), :]
        return remote(ref, ref, wsend.at[p], wrecv.at[p, sem], to)

    def relay_in(p, side):
        off, num = HALF[1 + side]
        return remote(
            ow.at[p, b, pl.ds(off, num), :], rb.at[p, side, pl.ds(0, num), :],
            wsend.at[p], wrecv.at[p, 2 + side], (to_xq, to_xn)[side],
        )

    def relay_out(p, side, xx):
        src = rb.at[p, side, pl.ds(0, HALF[1 + side][1]), :]
        return wx(p, src, xx, 1 + side, 4 + side, (to_xn, to_xq)[side])

    def whole(p, side, xx):
        return wx(p, ow.at[p, nb], xx, 0, side, (to_xq, to_xn)[side])

    def wz_out(p, j):
        for i in range(2):
            wz(p, z, j, 0, 6 + 2 * j + i, to_z[i]).start()

    def _wr(p):
        need_w(p)
        relay_in(p, 0).start()
        relay_in(p, 1).start()

    def _ww(p):
        need_w(p)
        whole(p, 0, x).start()
        whole(p, 1, x).start()

    def _wz0(p):
        need_w(p)
        wz_out(p, 0)

    def _wf(p, side):
        relay_in(p, side).wait_recv()
        relay_out(p, side, (xq, xn)[side]).start()

    def _wzx(p, j):
        whole(p, j - 1, XJ[j]).wait_recv()
        wz_out(p, j)

    def _wzo(p):
        relay_out(p, 0, xo).wait_recv()
        relay_out(p, 1, xo).wait_recv()
        wz_out(p, 3)

    def _wfw(p, j, i):
        zz = nxt(z, (-1, 1)[i])
        wz(p, zz, j, 0, 6 + 2 * j + i, to_z[i]).wait_recv()
        wz(p, zz, j, 1 + i, 14 + 2 * j + i, to_z[i]).start()

    def _wl(p):
        for j in range(4):
            for i in range(2):
                wz(p, nxt(z, 2), j, 1 + i, 14 + 2 * j + i, to_z[i]).wait_recv()

    AX = ((xq, xn), (xq, xn), (1, 0), xo, OX)
    AZ = ((nxt(z, 1), nxt(z, -1)), (nxt(z, -1), nxt(z, 1)), (0, 1), nxt(z, 2), OZ)
    AXES = ((AX, AZ), (AZ, AX))
    HERE = ((x, z), (z, x))

    def first_of(col, j):
        axis = AXES[col][0]
        return (HERE[col][0], axis[1][0], axis[1][1], axis[3])[j]

    def ocopy(col, f, s, part, sem, to_f, to_s):
        off, num = (0, ON[col]) if part is None else part
        row = (s * 4 + f) * ON[col] + off
        ref = (oa, ob)[col].at[pl.ds(pl.multiple_of(row, 16), num), :]
        to = dev(to_s * 4 + to_f if col == 0 else to_f * 4 + to_s)
        return remote(ref, ref, osend.at[col], orecv.at[col, sem], to)

    def _o0(col, i):
        need(2, loads2)
        f, s = HERE[col]
        ocopy(col, f, s, None, i, AXES[col][0][0][i], s).start()

    def _o1(col, i):
        send, recv, way, _, parts = AXES[col][0]
        s, w = HERE[col][1], way[i]
        ocopy(col, recv[i], s, None, i, send[i], s).wait_recv()
        if parts[col][w][1]:
            ocopy(col, recv[i], s, parts[col][w], 2 + w, send[w], s).start()

    def _o3(col):
        send, _, _, far, parts = AXES[col][0]
        s = HERE[col][1]
        for w in range(2):
            if parts[col][w][1]:
                ocopy(col, far, s, parts[col][w], 2 + w, send[w], s).wait_recv()

    def _os(col, j, i):
        need(2, loads2)
        f, s = HERE[col]
        ocopy(col, first_of(col, j), s, None, 4 + 2 * j + i, f, AXES[col][1][0][i]).start()

    def _of(col, j, i):
        send, recv, way, _, parts = AXES[col][1]
        f, w = HERE[col][0], way[i]
        fj = first_of(col, j)
        ocopy(col, fj, recv[i], None, 4 + 2 * j + i, f, send[i]).wait_recv()
        if parts[col][w][1]:
            ocopy(col, fj, recv[i], parts[col][w], 12 + 2 * j + w, f, send[w]).start()

    def ofar(col):
        send, _, _, far, parts = AXES[col][1]
        f = HERE[col][0]
        for j in range(4):
            for w in range(2):
                if parts[col][w][1]:
                    ocopy(
                        col, first_of(col, j), far, parts[col][w], 12 + 2 * j + w, f, send[w]
                    ).wait_recv()

    CC = (b, nb)

    def xcopy(cc, yy, kk, part, sem, to):
        off, num = ((0, SUB), (0, SUB // 2), (SUB // 2, SUB // 2))[part]
        row = CC[cc] * TOK + (yy * 2 + kk) * SUB + off
        ref = xs.at[pl.ds(pl.multiple_of(row, 16), num), :]
        return remote(ref, ref, xsend, xrecv.at[sem], to)

    to_y = (to_yp, to_ym)

    def xsem(cc, k):
        return cc * 12 + k

    def _xp(h):
        xcopy(0, y, core, 1 + h, 24 + h, to_xq).start()

    def xout(cc, h):
        for i in range(2):
            xcopy(cc, y, core, 1 + h, xsem(cc, 2 * i + h), to_y[i]).start()
        xcopy(cc, y, core, 1 + h, xsem(cc, 6 + h), to_pt).start()

    def _xo(h):
        xout(0, h)

    def _xg(h):
        xcopy(1, y, core, 1 + h, 24 + h, to_xq).wait_recv()
        xout(1, h)

    YB = (ym, yp)

    def _xf(cc, i):
        xcopy(cc, YB[i], core, 1 + i, xsem(cc, 3 * i), to_y[i]).wait_recv()
        xcopy(cc, YB[i], core, 1 + i, xsem(cc, 4 + i), to_y[i]).start()

    def _xm(cc, i):
        xcopy(cc, YB[i], core, 2 - i, xsem(cc, 1 + i), to_y[i]).wait_recv()
        xcopy(cc, YB[i], core, 0, xsem(cc, 8 + i), to_pt).start()

    def _xt(cc, i):
        xcopy(cc, yo, core, 1 + i, xsem(cc, 4 + i), to_y[i]).wait_recv()
        xcopy(cc, yo, core, 1 + i, xsem(cc, 10 + i), to_pt).start()

    def _xd(g):
        cc = (0, 1, 1)[g]
        if g < 2:
            xcopy(cc, y, other, 1, xsem(cc, 6), to_pt).wait_recv()
            xcopy(cc, y, other, 2, xsem(cc, 7), to_pt).wait_recv()
            xcopy(cc, ym, other, 0, xsem(cc, 8), to_pt).wait_recv()
            xcopy(cc, yp, other, 0, xsem(cc, 9), to_pt).wait_recv()
        if g != 1:
            xcopy(cc, yo, other, 1, xsem(cc, 10), to_pt).wait_recv()
            xcopy(cc, yo, other, 2, xsem(cc, 11), to_pt).wait_recv()

    base = WINDOW + (c - b) * TOK

    def _ang():
        def angle(i, carry):
            rows = pl.ds(pl.multiple_of(i * 128, 128), 128)
            pos = lax.broadcasted_iota(jnp.int32, (128, HD), 0) + (base + i * 128)
            a = pos.astype(F32) * freq_v[...]
            lane = lax.broadcasted_iota(jnp.int32, (128, HD), 1)
            cos[rows, :] = jnp.cos(a)
            sn = jnp.sin(a)
            sin[rows, :] = jnp.where(lane < HD // 2, -sn, sn)
            return carry

        lax.fori_loop(0, PAIR // 128, angle, 0)

    BLOCKS = (None, (y, ym, yp), (yo,))

    def tokens(g, i):
        return CC[0] * TOK + i * 128 if g == 0 else CC[1] * TOK + BLOCKS[g][i] * 128

    def at(start):
        return pl.ds(pl.multiple_of(start, 128), 128)

    def mm(w, g):
        num = (TOK, 384, 128)[g]

        def part(i, carry):
            ks = pl.ds(pl.multiple_of(i * KT, 128), KT)
            if g == 0:
                rows = xs[pl.ds(pl.multiple_of(CC[0] * TOK, TOK), TOK), ks]
            else:
                rows = [xs[at(tokens(g, k)), ks] for k in range(num // 128)]
                rows = jnp.concatenate(rows, axis=0) if num > 128 else rows[0]
            acc[0:num] += jnp.dot(rows, w[ks, :], preferred_element_type=F32)
            return carry

        acc[0:num] = jnp.zeros((num, 256), F32)
        lax.fori_loop(0, D // KT, part, 0)

    def each(g, fn):
        if g == 0:

            def go(i, carry):
                fn(pl.multiple_of(i * 128, 128), tokens(0, i))
                return carry

            lax.fori_loop(0, 4, go, 0)
        else:
            for i in range((0, 3, 1)[g]):
                fn(i * 128, tokens(g, i))

    def headed(row, tok, c0, gain):
        raw = acc[pl.ds(row, 128), c0:c0 + HD]
        r = lax.rsqrt(jnp.mean(raw * raw, axis=-1, keepdims=True) + EPSILON)
        n = raw * r * gain[...]
        return n * cos[at(tok), :] + pltpu.roll(n, HD // 2, 1) * sin[at(tok), :]

    def krows(m, cc):
        if m == 0:
            return 0, CC[cc] * TOK, TOK
        blk = (y, ym, yp, yo)[m - 1]
        return blk * 128, CC[1 - cc] * TOK + blk * 128, 128

    def kcopy(m, i):
        slot, row, num = krows(m, 0)
        return remote(
            kv.at[i, pl.ds(pl.multiple_of(WINDOW + row, 128), num), :],
            kr.at[0 if m == 0 else 1, i, pl.ds(pl.multiple_of(slot, 128), num), :],
            krsend.at[i, m], krrecv.at[i, m], (to_xq, to_xn)[i],
        )

    def kfinal(m, i, cc, to):
        slot, row, num = krows(m, cc)
        return remote(
            kr.at[0 if m == 0 else 1, i, pl.ds(pl.multiple_of(slot, 128), num), :],
            kv.at[i, pl.ds(pl.multiple_of(row, 128), num), :],
            kfsend.at[i, m], kfrecv.at[i, m], to,
        )

    def _mk(g):
        mm(w0, g)

        def keys(row, tok):
            kv[0, at(WINDOW + tok), :] = headed(row, tok, 0, kg_v).astype(BF)
            kv[1, at(WINDOW + tok), :] = acc[pl.ds(row, 128), HD:2 * HD].astype(BF)

        each(g, keys)

        @pl.when(c < 14)
        def _():
            for m in ((0,), (1, 2, 3), (4,))[g]:
                for i in range(2):
                    kcopy(m, i).start()

    def _kvf(m, i):
        src = (cq, cn)[i]

        @pl.when(src < 14)
        def _():
            kcopy(m, i).wait_recv()
            kfinal(m, i, 1, dev((src + 2) % 16)).start()

    def _mq(g):
        mm(w1, g)

        def queries(row, tok):
            for h in range(2):
                q = headed(row, tok, h * HD, qg_v) * QUERY_FACTOR
                qb[h, at(tok), :] = q.astype(BF)

        each(g, queries)

    def _aw():
        @pl.when(c < 2)
        def _():
            prior(0).wait()
            prior(1).wait()

        @pl.when(c >= 2)
        def _():
            for m in range(5):
                for i in range(2):
                    kfinal(m, i, 0, to_xq).wait_recv()

    first = WINDOW - start_s[0] - (c - b) * TOK

    def attend(q0):
        q = qb[:, pl.ds(q0, 128), :].reshape(256, HD)
        k = kv[0, pl.ds(q0, 1152), :]
        v = kv[1, pl.ds(q0, 1152), :]
        s = lax.dot_general(q, k, (((1,), (1,)), ((), ())), preferred_element_type=F32)
        j = lax.broadcasted_iota(jnp.int32, (256, 1152), 1)
        r = lax.broadcasted_iota(jnp.int32, (256, 1152), 0)
        r = jnp.where(r >= 128, r - 128, r)
        s = jnp.where((j > r) & (j <= r + WINDOW) & (j >= first - q0), s, F32(-1e30))
        m = jnp.max(s, axis=-1, keepdims=True)
        e = jnp.exp(s - m)
        total = jnp.sum(e, axis=-1, keepdims=True)
        return (jnp.dot(e.astype(BF), v, preferred_element_type=F32) / total).astype(BF)

    def swap(i, from_pair):
        rows = pl.ds(i * 128, 128)
        half = nb if from_pair else b
        return remote(ast.at[rows, :], att.at[half, rows, :], swsend.at[i], swrecv.at[i], to_xq)

    def _au(i):
        o = attend(pl.multiple_of(nb * TOK + i * 128, 128))
        ast[i * 128:(i + 1) * 128, 0:128] = o[:128]
        ast[i * 128:(i + 1) * 128, 128:256] = o[128:]
        swap(i, False).start()

    def _ao(i):
        o = attend(pl.multiple_of(b * TOK + i * 128, 128))
        att[b, i * 128:(i + 1) * 128, 0:128] = o[:128]
        att[b, i * 128:(i + 1) * 128, 128:256] = o[128:]

    def _sw():
        for i in range(4):
            swap(i, True).wait_recv()

    CHUNKS = [(0, 0), (1, 0), (0, 1), (0, 2), (1, 1), (1, 2), (0, 3), (1, 3)]

    def at_s(q):
        col, j = CHUNKS[q]
        axis = AXES[col][1]
        return (HERE[col][1], axis[1][0], axis[1][1], axis[3])[j]

    def wide(q):
        return pl.ds(0, CWP[CHUNKS[q][0]])

    def rcopy(src, dst, q, sem, to):
        return remote(src, dst, rsend.at[q, sem], rrecv.at[q, sem], to)

    def r0copy(q):
        return rcopy(pp.at[q, :, other, :, wide(q)], dd.at[q, :, :, wide(q)], q, 0, to_pt)

    def r1copy(q, half):
        return rcopy(
            cb.at[q, 0, pl.ds(half * 32, 32), wide(q)], ee.at[q, half, :, wide(q)], q, 1 + half,
            to_y[half],
        )

    def r2copy(q, half):
        return rcopy(
            cb.at[q, 1 + half, :, wide(q)], gg.at[q, half, :, wide(q)], q, 3 + half, to_y[half],
        )

    def both(q, yy):
        w = CWP[CHUNKS[q][0]]
        return pp[q, yy, core, :, 0:w].astype(F32) + dd[q, yy, :, 0:w].astype(F32)

    def _pj(q):
        col, j = CHUNKS[q]
        if j == 3:
            ofar(col)
        n = CW[col]
        wref = (oa, ob)[col]
        rows = pl.ds(pl.multiple_of(at_s(q) * n, 16), n)

        def part(i, carry):
            tok = pl.ds(pl.multiple_of(i * 256, 256), 256)
            o = None
            for h in range(2):
                d = lax.dot_general(
                    att[h, tok, :], wref[rows, h * 256:(h + 1) * 256],
                    (((1,), (1,)), ((), ())), preferred_element_type=F32,
                )
                o = d if o is None else o + d
            o = o.astype(BF)
            for g in range(4):
                pp[q, i * 2 + g // 2, g % 2, :, 0:n] = o[g * SUB:(g + 1) * SUB]
            return carry

        lax.fori_loop(0, 2, part, 0)
        r0copy(q).start()

    def _r1(q):
        w = CWP[CHUNKS[q][0]]
        r0copy(q).wait_recv()
        cb[q, 0, :, 0:w] = both(q, yo).astype(BF)
        r1copy(q, 0).start()
        r1copy(q, 1).start()

    def _r2(q, i):
        w = CWP[CHUNKS[q][0]]
        r1copy(q, i).wait_recv()
        a = both(q, (yp, ym)[i])
        add = slice(32 * i, 32 * i + 32)
        rest = slice(32 - 32 * i, 64 - 32 * i)
        cb[q, 1 + i, add, 0:w] = (a[add] + ee[q, i, :, 0:w].astype(F32)).astype(BF)
        cb[q, 1 + i, rest, 0:w] = a[rest].astype(BF)
        r2copy(q, i).start()

    def _r3(q):
        w = CWP[CHUNKS[q][0]]
        r2copy(q, 0).wait_recv()
        r2copy(q, 1).wait_recv()
        v = both(q, y) + gg[q, 0, :, 0:w].astype(F32) + gg[q, 1, :, 0:w].astype(F32)
        (sa, sb)[CHUNKS[q][0]][at_s(q)] = v

    for fn, *nums in (
        (_wz0, 1), (_o0, 1, 0), (_ww, 0), (_o0, 1, 1), (_os, 1, 0, 1), (_xp, 0), (_wr, 0),
        (_o0, 0, 1), (_xo, 0), (_xp, 1), (_wzx, 0, 2), (_wr, 1), (_xo, 1), (_wz0, 0),
        (_o1, 1, 1), (_o1, 1, 0), (_wzx, 0, 1), (_wf, 0, 1), (_ww, 1), (_xg, 0), (_wf, 1, 1),
        (_wfw, 0, 0, 0), (_os, 1, 2, 1), (_wf, 0, 0), (_ang,), (_o1, 0, 1),
        (_wfw, 0, 2, 1), (_os, 1, 1, 1), (_wfw, 0, 0, 1), (_wfw, 0, 2, 0), (_wzx, 1, 2),
        (_xg, 1), (_xf, 0, 0), (_wf, 1, 0), (_o0, 0, 0), (_xf, 0, 1), (_xf, 1, 0), (_wzo, 0),
        (_wzx, 1, 1), (_os, 1, 1, 0), (_wfw, 0, 1, 1), (_wfw, 0, 1, 0), (_wfw, 0, 3, 0),
        (_wfw, 1, 2, 0), (_xm, 1, 0), (_xf, 1, 1), (_o3, 1), (_xm, 1, 1), (_os, 1, 2, 0),
        (_wfw, 0, 3, 1), (_os, 1, 3, 1), (_os, 1, 3, 0), (_of, 1, 0, 1), (_wfw, 1, 2, 1),
        (_xd, 1), (_xm, 0, 0), (_wzo, 1), (_wfw, 1, 0, 1), (_o1, 0, 0), (_wfw, 1, 0, 0),
        (_wl, 0), (_xt, 0, 0), (_of, 1, 2, 1), (_xm, 0, 1), (_wfw, 1, 1, 0), (_xt, 0, 1),
        (_mk, 1), (_xd, 0), (_wfw, 1, 1, 1), (_mk, 0), (_kvf, 2, 1), (_kvf, 2, 0),
        (_wfw, 1, 3, 1), (_of, 1, 1, 1), (_os, 0, 0, 1), (_wfw, 1, 3, 0), (_xt, 1, 0),
        (_xt, 1, 1), (_o3, 0), (_kvf, 3, 0), (_os, 0, 3, 0), (_kvf, 3, 1), (_xd, 2), (_mk, 2),
        (_os, 0, 0, 0), (_os, 0, 1, 0), (_kvf, 0, 0), (_os, 0, 1, 1), (_of, 1, 3, 1),
        (_kvf, 0, 1), (_os, 0, 3, 1), (_kvf, 1, 0), (_kvf, 1, 1), (_wl, 1), (_mq, 0),
        (_kvf, 4, 1), (_kvf, 4, 0), (_mq, 1), (_mq, 2), (_aw,), (_au, 0), (_au, 1), (_au, 2),
        (_os, 0, 2, 1), (_au, 3), (_of, 0, 1, 1), (_of, 1, 2, 0), (_ao, 0), (_os, 0, 2, 0),
        (_ao, 1), (_of, 0, 0, 1), (_of, 0, 3, 0), (_os, 1, 0, 0), (_of, 0, 3, 1), (_ao, 2),
        (_ao, 3), (_sw,), (_pj, 1), (_pj, 0), (_pj, 5), (_r1, 1), (_of, 0, 2, 1), (_pj, 3),
        (_r1, 0), (_of, 1, 0, 0), (_r1, 5), (_of, 0, 1, 0), (_of, 1, 1, 0), (_of, 0, 0, 0),
        (_of, 0, 2, 0), (_of, 1, 3, 0), (_r1, 3), (_r2, 1, 0), (_r2, 1, 1), (_r2, 0, 0),
        (_pj, 4), (_r2, 5, 1), (_pj, 2), (_r1, 4), (_r2, 3, 0), (_r2, 3, 1), (_r1, 2),
        (_pj, 6), (_r2, 4, 0), (_r2, 0, 1), (_r3, 1), (_r1, 6), (_r2, 4, 1), (_r2, 5, 0),
        (_pj, 7), (_r1, 7), (_r2, 2, 1), (_r3, 0), (_r3, 3), (_r2, 6, 0), (_r2, 2, 0),
        (_r2, 6, 1), (_r2, 7, 1), (_r2, 7, 0), (_r3, 2), (_r3, 6), (_r3, 5), (_r3, 4),
        (_r3, 7),
    ):
        fn(*nums)

    for i in range(16):
        zi, xi = i // 4, i % 4
        full[:, i * BLK:i * BLK + ON[0]] = sa[zi, :, xi * ON[0]:(xi + 1) * ON[0]]
        full[:, i * BLK + ON[0]:(i + 1) * BLK] = sb[xi, :, zi * ON[1]:(zi + 1) * ON[1]]

    def final(i, carry):
        rows = pl.ds(pl.multiple_of(i * 16, 16), 16)
        v = full[rows, :]
        r = lax.rsqrt(jnp.mean(v * v, axis=-1, keepdims=True) + EPSILON)
        out_v[rows, :] = (hid[rows, :].astype(F32) + v * r * post[...]).astype(BF)
        return carry

    lax.fori_loop(0, SUB // 16, final, 0)

    for p in range(2):
        remote(ws[p], ws[p], wsend.at[p], wrecv.at[p, 0], to_pt).wait_send()
    for col in range(2):
        ref = (oa, ob)[col].at[pl.ds(0, 15 * ON[col]), :]
        remote(ref, ref, osend.at[col], orecv.at[col, 0], to_pt).wait_send()
    ref = xs.at[pl.ds(0, 15 * SUB), :]
    remote(ref, ref, xsend, xrecv.at[0], to_pt).wait_send()
    for m in range(5):
        for i in range(2):

            @pl.when(c < 14)
            def _():
                kcopy(m, i).wait_send()

            @pl.when((cq, cn)[i] < 14)
            def _():
                kfinal(m, i, 1, to_xq).wait_send()

    for i in range(4):
        swap(i, False).wait_send()
    for q in range(8):
        r0copy(q).wait_send()
        for half in range(2):
            r1copy(q, half).wait_send()
            r2copy(q, half).wait_send()


def local(
    hidden_in, stretch_start, pre_gain, q_weight, k_weight, v_weight, o_weight, q_gain, k_gain,
    prior_keys, prior_values, post_gain,
):
    frequency = 10000.0 ** (-jnp.arange(HD // 2, dtype=F32) / (HD // 2))
    freq2 = jnp.concatenate([frequency, frequency]).reshape(1, HD)
    hbm = pl.BlockSpec(memory_space=pl.ANY)
    vm = pl.BlockSpec(memory_space=pltpu.VMEM)
    sm = pl.BlockSpec(memory_space=pltpu.SMEM)
    dma = pltpu.SemaphoreType.DMA
    return pl.pallas_call(
        body,
        out_shape=jax.ShapeDtypeStruct((SUB, D), BF),
        in_specs=[hbm, sm, hbm, hbm, hbm, hbm, hbm, vm, vm, hbm, hbm, hbm, vm],
        out_specs=vm,
        scratch_shapes=[
            pltpu.VMEM((D, 256), BF), pltpu.VMEM((D, 256), BF),
            pltpu.VMEM((16 * ON[0], 512), BF), pltpu.VMEM((16 * ON[1], 512), BF),
            pltpu.VMEM((2, 2, BLK, 256), BF), pltpu.VMEM((2, 2, 176, 256), BF),
            pltpu.VMEM((PAIR, D), BF),
            pltpu.VMEM((2, WINDOW + PAIR, HD), BF), pltpu.VMEM((2, 2, TOK, HD), BF),
            pltpu.VMEM((2, PAIR, HD), BF),
            pltpu.VMEM((2, TOK, 256), BF), pltpu.VMEM((TOK, 256), BF),
            pltpu.VMEM((TOK, 256), F32),
            pltpu.VMEM((SUB, D), BF), pltpu.VMEM((1, D), F32), pltpu.VMEM((1, D), F32),
            pltpu.VMEM((PAIR, HD), F32), pltpu.VMEM((PAIR, HD), F32),
            pltpu.VMEM((8, 4, 2, SUB, 768), BF),
            pltpu.VMEM((8, 4, SUB, 768), BF),
            pltpu.VMEM((8, 2, SUB // 2, 768), BF),
            pltpu.VMEM((8, 2, SUB, 768), BF),
            pltpu.VMEM((8, 3, SUB, 768), BF),
            pltpu.VMEM((4, SUB, CWP[0]), F32), pltpu.VMEM((4, SUB, CWP[1]), F32),
            pltpu.VMEM((SUB, D), F32),
            dma((16,)), dma((2,)), dma((2, 22)), dma((2,)), dma((2, 20)), dma, dma((26,)),
            dma((2, 5)), dma((2, 5)), dma((2, 5)), dma((2, 5)), dma((4,)), dma((4,)),
            dma((8, 5)), dma((8, 5)),
        ],
        compiler_params=pltpu.CompilerParams(
            collective_id=0, has_side_effects=True, vmem_limit_bytes=64 * 1024 * 1024 - 128 * 1024
        ),
        name="layer",
    )(
        hidden_in, stretch_start, pre_gain, q_weight, k_weight, v_weight,
        o_weight.T, q_gain.reshape(1, HD), k_gain.reshape(1, HD), prior_keys, prior_values,
        post_gain, freq2,
    )


def solution(mesh):
    return jax.shard_map(
        local,
        mesh=mesh,
        in_specs=(
            P(("ctx", "tp"), None), P(), P(), P("ctx", "tp"), P("ctx", "tp"), P("ctx", "tp"),
            P("tp", "ctx"), P(), P(), P(None, "tp"), P(None, "tp"), P(),
        ),
        out_specs=P(("ctx", "tp"), None),
        check_vma=False,
    )
```

```python
import jax
import jax.numpy as jnp
from jax import lax
from jax.experimental import pallas as pl
from jax.experimental.pallas import tpu as pltpu
from jax.sharding import PartitionSpec as P

HD = 128
WINDOW = 1024
EPSILON = 1e-06
QUERY_FACTOR = 168.0 ** (-0.5)
MESH = pl.DeviceIdType.MESH

D = 5376
BLK = 336
TOK = 512
PAIR = 1024
SUB = 64
HALF = (0, 336), (0, 176), (176, 160)
ON = (192, 144)
OX = ((0, 0), (0, 192)), ((0, 0), (0, 144))
OZ = ((0, 96), (96, 96)), ((0, 80), (80, 64))
CW = (768, 576)
CWP = (768, 640)
KT = 768
BF = jnp.bfloat16
F32 = jnp.float32


def body(
    hid_h, start_s, pre_h, q_h, k_h, v_h, o_h, qg_v, kg_v, pk_h, pv_h, post_h, freq_v,
    out_v,
    w0, w1, oa, ob, ow, rb, xs, kv, kr, qb, att, ast, acc, hid, pre, post, cos, sin,
    pp, dd, ee, gg, cb, sa, sb, full,
    lsem, wsend, wrecv, osend, orecv, xsend, xrecv, krsend, krrecv, kfsend, kfrecv,
    swsend, swrecv, rsend, rrecv,
):
    c = lax.axis_index("ctx")
    t = lax.axis_index("tp")
    z, x = c // 4, c % 4
    y, core = t // 2, t % 2
    b = x % 2
    nb = 1 - b
    ws = (w0, w1)

    def nxt(a, d):
        return (a + d + 4) % 4

    def pairx(xx):
        return xx + 1 - 2 * (xx % 2)

    def otherx(xx):
        return (xx + 3 + 2 * (xx % 2)) % 4

    xq, xn, xo = pairx(x), otherx(x), nxt(x, 2)
    yp, ym, yo = nxt(y, 1), nxt(y, -1), nxt(y, 2)
    other = 1 - core
    to_yp = {"ctx": c, "tp": yp * 2 + core}
    to_ym = {"ctx": c, "tp": ym * 2 + core}
    to_pt = {"ctx": c, "tp": y * 2 + other}

    def dev(ci):
        return {"ctx": ci, "tp": t}

    to_xq, to_xn = dev(z * 4 + xq), dev(z * 4 + xn)
    to_zp, to_zm = dev(nxt(z, 1) * 4 + x), dev(nxt(z, -1) * 4 + x)

    def remote(src, dst, ssem, rsem, to):
        return pltpu.make_async_remote_copy(
            src_ref=src, dst_ref=dst, send_sem=ssem, recv_sem=rsem, device_id=to,
            device_id_type=MESH,
        )

    cq, cn = z * 4 + xq, z * 4 + xn
    behind = (c + 14) % 16
    zb, xb = behind // 4, behind % 4
    barrier = pltpu.get_barrier_semaphore()
    peers = [to_yp, to_ym, to_pt, to_xq, to_xn, to_zp, to_zm]
    peers += [dev((cq + 2) % 16), dev((cn + 2) % 16)]
    peers += [dev(zb * 4 + pairx(xb)), dev(zb * 4 + otherx(xb))]
    for peer in peers:
        pl.semaphore_signal(barrier, inc=1, device_id=peer, device_id_type=MESH)

    own = pl.ds(pl.multiple_of(c * BLK, 16), BLK)
    hc = pl.ds(pl.multiple_of(b * HD, HD), HD)
    lo, hi = pl.ds(0, HD), pl.ds(HD, HD)
    loads0 = [
        pltpu.make_async_copy(k_h.at[:, lo], ow.at[0, 0, :, lo], lsem.at[0]),
        pltpu.make_async_copy(v_h.at[:, lo], ow.at[0, 0, :, hi], lsem.at[1]),
        pltpu.make_async_copy(k_h.at[:, hi], ow.at[0, 1, :, lo], lsem.at[2]),
        pltpu.make_async_copy(v_h.at[:, hi], ow.at[0, 1, :, hi], lsem.at[3]),
        pltpu.make_async_copy(k_h.at[:, hc], w0.at[own, lo], lsem.at[4]),
        pltpu.make_async_copy(v_h.at[:, hc], w0.at[own, hi], lsem.at[5]),
    ]
    loadx = [
        pltpu.make_async_copy(hid_h, hid, lsem.at[6]),
        pltpu.make_async_copy(pre_h, pre.at[0], lsem.at[7]),
    ]
    loads1 = [
        pltpu.make_async_copy(q_h.at[:, pl.ds(0, 256)], ow.at[1, 0], lsem.at[8]),
        pltpu.make_async_copy(q_h.at[:, pl.ds(256, 256)], ow.at[1, 1], lsem.at[9]),
        pltpu.make_async_copy(
            q_h.at[:, pl.ds(pl.multiple_of(b * 256, 256), 256)], w1.at[own, :], lsem.at[10]
        ),
    ]
    loads2 = [
        pltpu.make_async_copy(
            o_h.at[pl.ds(0, ON[0]), :],
            oa.at[pl.ds(pl.multiple_of(c * ON[0], 16), ON[0]), :], lsem.at[11],
        ),
        pltpu.make_async_copy(
            o_h.at[pl.ds(ON[0], ON[1]), :],
            ob.at[pl.ds(pl.multiple_of((x * 4 + z) * ON[1], 16), ON[1]), :], lsem.at[12],
        ),
        pltpu.make_async_copy(post_h, post.at[0], lsem.at[13]),
    ]
    for load in loadx + loads0 + loads1 + loads2:
        load.start()

    def prior(i):
        return pltpu.make_async_copy(
            (pk_h, pv_h)[i].at[:, hc], kv.at[i, pl.ds(0, WINDOW), :], lsem.at[14 + i]
        )

    @pl.when(c < 2)
    def _():
        prior(0).start()
        prior(1).start()

    for load in loadx:
        load.wait()

    def prenorm(i, carry):
        rows = pl.ds(pl.multiple_of(i * 16, 16), 16)
        h = hid[rows, :].astype(F32)
        r = lax.rsqrt(jnp.mean(h * h, axis=-1, keepdims=True) + EPSILON)
        to = pl.ds(pl.multiple_of(b * TOK + t * SUB + i * 16, 16), 16)
        xs[to, :] = (h * r * pre[...]).astype(BF)
        return carry

    lax.fori_loop(0, SUB // 16, prenorm, 0)
    for q in (1, 4, 5, 7):
        for g in range(8):
            pp[q, g // 2, g % 2, :, 512:640] = jnp.zeros((SUB, 128), BF)
    base = WINDOW + (c - b) * TOK

    def angle(i, carry):
        rows = pl.ds(pl.multiple_of(i * 128, 128), 128)
        pos = lax.broadcasted_iota(jnp.int32, (128, HD), 0) + (base + i * 128)
        a = pos.astype(F32) * freq_v[...]
        lane = lax.broadcasted_iota(jnp.int32, (128, HD), 1)
        cos[rows, :] = jnp.cos(a)
        sn = jnp.sin(a)
        sin[rows, :] = jnp.where(lane < HD // 2, -sn, sn)
        return carry

    lax.fori_loop(0, PAIR // 128, angle, 0)

    pl.semaphore_wait(barrier, len(peers))

    waited = set()

    def need(name, group):
        if name not in waited:
            waited.add(name)
            for load in group:
                load.wait()

    def need_w(p):
        need(p, (loads0, loads1)[p])

    XJ = (x, xq, xn, xo)
    to_z = (to_zp, to_zm)

    def wrows(zz, xx, part):
        off, num = HALF[part]
        return pl.ds(pl.multiple_of((zz * 4 + xx) * BLK + off, 16), num)

    def wx(p, src, xx, part, sem, to):
        return remote(
            src, ws[p].at[wrows(z, xx, part), :], wsend.at[p], wrecv.at[p, sem], to
        )

    def wz(p, zz, j, part, sem, to):
        ref = ws[p].at[wrows(zz, XJ[j], part), :]
        return remote(ref, ref, wsend.at[p], wrecv.at[p, sem], to)

    def relay_in(p, side):
        off, num = HALF[1 + side]
        return remote(
            ow.at[p, b, pl.ds(off, num), :], rb.at[p, side, pl.ds(0, num), :],
            wsend.at[p], wrecv.at[p, 2 + side], (to_xq, to_xn)[side],
        )

    def relay_out(p, side, xx):
        src = rb.at[p, side, pl.ds(0, HALF[1 + side][1]), :]
        return wx(p, src, xx, 1 + side, 4 + side, (to_xn, to_xq)[side])

    def whole(p, side, xx):
        return wx(p, ow.at[p, nb], xx, 0, side, (to_xq, to_xn)[side])

    def wz_out(p, j):
        for i in range(2):
            wz(p, z, j, 0, 6 + 2 * j + i, to_z[i]).start()

    def _wr(p):
        need_w(p)
        relay_in(p, 0).start()
        relay_in(p, 1).start()

    def _ww(p):
        need_w(p)
        whole(p, 0, x).start()
        whole(p, 1, x).start()

    def _wz0(p):
        need_w(p)
        wz_out(p, 0)

    def _wf(p, side):
        relay_in(p, side).wait_recv()
        relay_out(p, side, (xq, xn)[side]).start()

    def _wzx(p, j):
        whole(p, j - 1, XJ[j]).wait_recv()
        wz_out(p, j)

    def _wzo(p):
        relay_out(p, 0, xo).wait_recv()
        relay_out(p, 1, xo).wait_recv()
        wz_out(p, 3)

    def _wfw(p, j, i):
        zz = nxt(z, (-1, 1)[i])
        wz(p, zz, j, 0, 6 + 2 * j + i, to_z[i]).wait_recv()
        wz(p, zz, j, 1 + i, 14 + 2 * j + i, to_z[i]).start()

    def _wl(p):
        for j in range(4):
            for i in range(2):
                wz(p, nxt(z, 2), j, 1 + i, 14 + 2 * j + i, to_z[i]).wait_recv()

    AX = ((xq, xn), (xq, xn), (1, 0), xo, OX)
    AZ = ((nxt(z, 1), nxt(z, -1)), (nxt(z, -1), nxt(z, 1)), (0, 1), nxt(z, 2), OZ)
    AXES = ((AX, AZ), (AZ, AX))
    HERE = ((x, z), (z, x))

    def first_of(col, j):
        axis = AXES[col][0]
        return (HERE[col][0], axis[1][0], axis[1][1], axis[3])[j]

    def ocopy(col, f, s, part, sem, to_f, to_s):
        off, num = (0, ON[col]) if part is None else part
        row = (s * 4 + f) * ON[col] + off
        ref = (oa, ob)[col].at[pl.ds(pl.multiple_of(row, 16), num), :]
        to = dev(to_s * 4 + to_f if col == 0 else to_f * 4 + to_s)
        return remote(ref, ref, osend.at[col], orecv.at[col, sem], to)

    def _o0(col, i):
        need(2, loads2)
        f, s = HERE[col]
        ocopy(col, f, s, None, i, AXES[col][0][0][i], s).start()

    def _o1(col, i):
        send, recv, way, _, parts = AXES[col][0]
        s, w = HERE[col][1], way[i]
        ocopy(col, recv[i], s, None, i, send[i], s).wait_recv()
        if parts[col][w][1]:
            ocopy(col, recv[i], s, parts[col][w], 2 + w, send[w], s).start()

    def _o3(col):
        send, _, _, far, parts = AXES[col][0]
        s = HERE[col][1]
        for w in range(2):
            if parts[col][w][1]:
                ocopy(col, far, s, parts[col][w], 2 + w, send[w], s).wait_recv()

    def _os(col, j, i):
        need(2, loads2)
        f, s = HERE[col]
        ocopy(col, first_of(col, j), s, None, 4 + 2 * j + i, f, AXES[col][1][0][i]).start()

    def _of(col, j, i):
        send, recv, way, _, parts = AXES[col][1]
        f, w = HERE[col][0], way[i]
        fj = first_of(col, j)
        ocopy(col, fj, recv[i], None, 4 + 2 * j + i, f, send[i]).wait_recv()
        if parts[col][w][1]:
            ocopy(col, fj, recv[i], parts[col][w], 12 + 2 * j + w, f, send[w]).start()

    def ofar(col):
        send, _, _, far, parts = AXES[col][1]
        f = HERE[col][0]
        for j in range(4):
            for w in range(2):
                if parts[col][w][1]:
                    ocopy(
                        col, first_of(col, j), far, parts[col][w], 12 + 2 * j + w, f, send[w]
                    ).wait_recv()

    CC = (b, nb)

    def xcopy(cc, yy, kk, part, sem, to):
        off, num = ((0, SUB), (0, SUB // 2), (SUB // 2, SUB // 2))[part]
        row = CC[cc] * TOK + (yy * 2 + kk) * SUB + off
        ref = xs.at[pl.ds(pl.multiple_of(row, 16), num), :]
        return remote(ref, ref, xsend, xrecv.at[sem], to)

    to_y = (to_yp, to_ym)

    def xsem(cc, k):
        return cc * 12 + k

    def _xp(h):
        xcopy(0, y, core, 1 + h, 24 + h, to_xq).start()

    def xout(cc, h):
        for i in range(2):
            xcopy(cc, y, core, 1 + h, xsem(cc, 2 * i + h), to_y[i]).start()
        xcopy(cc, y, core, 1 + h, xsem(cc, 6 + h), to_pt).start()

    def _xo(h):
        xout(0, h)

    def _xg(h):
        xcopy(1, y, core, 1 + h, 24 + h, to_xq).wait_recv()
        xout(1, h)

    YB = (ym, yp)

    def _xf(cc, i):
        xcopy(cc, YB[i], core, 1 + i, xsem(cc, 3 * i), to_y[i]).wait_recv()
        xcopy(cc, YB[i], core, 1 + i, xsem(cc, 4 + i), to_y[i]).start()

    def _xm(cc, i):
        xcopy(cc, YB[i], core, 2 - i, xsem(cc, 1 + i), to_y[i]).wait_recv()
        xcopy(cc, YB[i], core, 0, xsem(cc, 8 + i), to_pt).start()

    def _xt(cc, i):
        xcopy(cc, yo, core, 1 + i, xsem(cc, 4 + i), to_y[i]).wait_recv()
        xcopy(cc, yo, core, 1 + i, xsem(cc, 10 + i), to_pt).start()

    def _xd(g):
        cc = (0, 1, 1)[g]
        if g < 2:
            xcopy(cc, y, other, 1, xsem(cc, 6), to_pt).wait_recv()
            xcopy(cc, y, other, 2, xsem(cc, 7), to_pt).wait_recv()
            xcopy(cc, ym, other, 0, xsem(cc, 8), to_pt).wait_recv()
            xcopy(cc, yp, other, 0, xsem(cc, 9), to_pt).wait_recv()
        if g != 1:
            xcopy(cc, yo, other, 1, xsem(cc, 10), to_pt).wait_recv()
            xcopy(cc, yo, other, 2, xsem(cc, 11), to_pt).wait_recv()

    BLOCKS = (None, (y, ym, yp), (yo,))

    def tokens(g, i):
        return CC[0] * TOK + i * 128 if g == 0 else CC[1] * TOK + BLOCKS[g][i] * 128

    def at(start):
        return pl.ds(pl.multiple_of(start, 128), 128)

    def mm(w, g):
        num = (TOK, 384, 128)[g]

        def part(i, carry):
            ks = pl.ds(pl.multiple_of(i * KT, 128), KT)
            if g == 0:
                rows = xs[pl.ds(pl.multiple_of(CC[0] * TOK, TOK), TOK), ks]
            else:
                rows = [xs[at(tokens(g, k)), ks] for k in range(num // 128)]
                rows = jnp.concatenate(rows, axis=0) if num > 128 else rows[0]
            acc[0:num] += jnp.dot(rows, w[ks, :], preferred_element_type=F32)
            return carry

        acc[0:num] = jnp.zeros((num, 256), F32)
        lax.fori_loop(0, D // KT, part, 0)

    def each(g, fn):
        if g == 0:

            def go(i, carry):
                fn(pl.multiple_of(i * 128, 128), tokens(0, i))
                return carry

            lax.fori_loop(0, 4, go, 0)
        else:
            for i in range((0, 3, 1)[g]):
                fn(i * 128, tokens(g, i))

    def headed(row, tok, c0, gain):
        raw = acc[pl.ds(row, 128), c0:c0 + HD]
        r = lax.rsqrt(jnp.mean(raw * raw, axis=-1, keepdims=True) + EPSILON)
        n = raw * r * gain[...]
        return n * cos[at(tok), :] + pltpu.roll(n, HD // 2, 1) * sin[at(tok), :]

    def krows(m, cc):
        if m == 0:
            return 0, CC[cc] * TOK, TOK
        blk = (y, ym, yp, yo)[m - 1]
        return blk * 128, CC[1 - cc] * TOK + blk * 128, 128

    def kcopy(m, i):
        slot, row, num = krows(m, 0)
        return remote(
            kv.at[i, pl.ds(pl.multiple_of(WINDOW + row, 128), num), :],
            kr.at[0 if m == 0 else 1, i, pl.ds(pl.multiple_of(slot, 128), num), :],
            krsend.at[i, m], krrecv.at[i, m], (to_xq, to_xn)[i],
        )

    def kfinal(m, i, cc, to):
        slot, row, num = krows(m, cc)
        return remote(
            kr.at[0 if m == 0 else 1, i, pl.ds(pl.multiple_of(slot, 128), num), :],
            kv.at[i, pl.ds(pl.multiple_of(row, 128), num), :],
            kfsend.at[i, m], kfrecv.at[i, m], to,
        )

    def _mk(g):
        mm(w0, g)

        def keys(row, tok):
            kv[0, at(WINDOW + tok), :] = headed(row, tok, 0, kg_v).astype(BF)
            kv[1, at(WINDOW + tok), :] = acc[pl.ds(row, 128), HD:2 * HD].astype(BF)

        each(g, keys)

        @pl.when(c < 14)
        def _():
            for m in ((0,), (1, 2, 3), (4,))[g]:
                for i in range(2):
                    kcopy(m, i).start()

    def _kvf(m, i):
        src = (cq, cn)[i]

        @pl.when(src < 14)
        def _():
            kcopy(m, i).wait_recv()
            kfinal(m, i, 1, dev((src + 2) % 16)).start()

    def _mq(g):
        mm(w1, g)

        def queries(row, tok):
            for h in range(2):
                q = headed(row, tok, h * HD, qg_v) * QUERY_FACTOR
                qb[h, at(tok), :] = q.astype(BF)

        each(g, queries)

    def _aw():
        @pl.when(c < 2)
        def _():
            prior(0).wait()
            prior(1).wait()

        @pl.when(c >= 2)
        def _():
            for m in range(5):
                for i in range(2):
                    kfinal(m, i, 0, to_xq).wait_recv()

    first = WINDOW - start_s[0] - (c - b) * TOK

    def attend(q0):
        q = qb[:, pl.ds(q0, 128), :].reshape(256, HD)
        k = kv[0, pl.ds(q0, 1152), :]
        v = kv[1, pl.ds(q0, 1152), :]
        s = lax.dot_general(q, k, (((1,), (1,)), ((), ())), preferred_element_type=F32)
        j = lax.broadcasted_iota(jnp.int32, (256, 1152), 1)
        r = lax.broadcasted_iota(jnp.int32, (256, 1152), 0)
        r = jnp.where(r >= 128, r - 128, r)
        s = jnp.where((j > r) & (j <= r + WINDOW) & (j >= first - q0), s, F32(-1e30))
        m = jnp.max(s, axis=-1, keepdims=True)
        e = jnp.exp(s - m)
        total = jnp.sum(e, axis=-1, keepdims=True)
        return (jnp.dot(e.astype(BF), v, preferred_element_type=F32) / total).astype(BF)

    def swap(i, from_pair):
        rows = pl.ds(i * 128, 128)
        half = nb if from_pair else b
        return remote(ast.at[rows, :], att.at[half, rows, :], swsend.at[i], swrecv.at[i], to_xq)

    def _au(i):
        o = attend(pl.multiple_of(nb * TOK + i * 128, 128))
        ast[i * 128:(i + 1) * 128, 0:128] = o[:128]
        ast[i * 128:(i + 1) * 128, 128:256] = o[128:]
        swap(i, False).start()

    def _ao(i):
        o = attend(pl.multiple_of(b * TOK + i * 128, 128))
        att[b, i * 128:(i + 1) * 128, 0:128] = o[:128]
        att[b, i * 128:(i + 1) * 128, 128:256] = o[128:]

    def _sw():
        for i in range(4):
            swap(i, True).wait_recv()

    CHUNKS = [(0, 0), (1, 0), (0, 1), (0, 2), (1, 1), (1, 2), (0, 3), (1, 3)]

    def at_s(q):
        col, j = CHUNKS[q]
        axis = AXES[col][1]
        return (HERE[col][1], axis[1][0], axis[1][1], axis[3])[j]

    def wide(q):
        return pl.ds(0, CWP[CHUNKS[q][0]])

    def rcopy(src, dst, q, sem, to):
        return remote(src, dst, rsend.at[q, sem], rrecv.at[q, sem], to)

    def r0copy(q):
        return rcopy(pp.at[q, :, other, :, wide(q)], dd.at[q, :, :, wide(q)], q, 0, to_pt)

    def r1copy(q, half):
        return rcopy(
            cb.at[q, 0, pl.ds(half * 32, 32), wide(q)], ee.at[q, half, :, wide(q)], q, 1 + half,
            to_y[half],
        )

    def r2copy(q, half):
        return rcopy(
            cb.at[q, 1 + half, :, wide(q)], gg.at[q, half, :, wide(q)], q, 3 + half, to_y[half],
        )

    def both(q, yy):
        w = CWP[CHUNKS[q][0]]
        return pp[q, yy, core, :, 0:w].astype(F32) + dd[q, yy, :, 0:w].astype(F32)

    def _pj(q):
        col, j = CHUNKS[q]
        if j == 3:
            ofar(col)
        n = CW[col]
        wref = (oa, ob)[col]
        rows = pl.ds(pl.multiple_of(at_s(q) * n, 16), n)

        def part(i, carry):
            tok = pl.ds(pl.multiple_of(i * 256, 256), 256)
            o = None
            for h in range(2):
                d = lax.dot_general(
                    att[h, tok, :], wref[rows, h * 256:(h + 1) * 256],
                    (((1,), (1,)), ((), ())), preferred_element_type=F32,
                )
                o = d if o is None else o + d
            o = o.astype(BF)
            for g in range(4):
                pp[q, i * 2 + g // 2, g % 2, :, 0:n] = o[g * SUB:(g + 1) * SUB]
            return carry

        lax.fori_loop(0, 2, part, 0)
        r0copy(q).start()

    def _r1(q):
        w = CWP[CHUNKS[q][0]]
        r0copy(q).wait_recv()
        cb[q, 0, :, 0:w] = both(q, yo).astype(BF)
        r1copy(q, 0).start()
        r1copy(q, 1).start()

    def _r2(q, i):
        w = CWP[CHUNKS[q][0]]
        r1copy(q, i).wait_recv()
        a = both(q, (yp, ym)[i])
        add = slice(32 * i, 32 * i + 32)
        rest = slice(32 - 32 * i, 64 - 32 * i)
        cb[q, 1 + i, add, 0:w] = (a[add] + ee[q, i, :, 0:w].astype(F32)).astype(BF)
        cb[q, 1 + i, rest, 0:w] = a[rest].astype(BF)
        r2copy(q, i).start()

    def _r3(q):
        w = CWP[CHUNKS[q][0]]
        r2copy(q, 0).wait_recv()
        r2copy(q, 1).wait_recv()
        v = both(q, y) + gg[q, 0, :, 0:w].astype(F32) + gg[q, 1, :, 0:w].astype(F32)
        (sa, sb)[CHUNKS[q][0]][at_s(q)] = v

    for fn, *nums in (
        (_wz0, 1), (_o0, 1, 0), (_ww, 0), (_o0, 1, 1), (_os, 1, 0, 1), (_xp, 0), (_wr, 0),
        (_o0, 0, 1), (_xo, 0), (_xp, 1), (_wzx, 0, 2), (_wr, 1), (_xo, 1), (_wz0, 0),
        (_o1, 1, 1), (_o1, 1, 0), (_wzx, 0, 1), (_wf, 0, 1), (_ww, 1), (_xg, 0), (_wf, 1, 1),
        (_wfw, 0, 0, 0), (_os, 1, 2, 1), (_wf, 0, 0), (_o1, 0, 1),
        (_wfw, 0, 2, 1), (_os, 1, 1, 1), (_wfw, 0, 0, 1), (_wfw, 0, 2, 0), (_wzx, 1, 2),
        (_xg, 1), (_xf, 0, 0), (_wf, 1, 0), (_o0, 0, 0), (_xf, 0, 1), (_xf, 1, 0), (_wzo, 0),
        (_wzx, 1, 1), (_os, 1, 1, 0), (_wfw, 0, 1, 1), (_wfw, 0, 1, 0), (_wfw, 0, 3, 0),
        (_wfw, 1, 2, 0), (_xm, 1, 0), (_xf, 1, 1), (_o3, 1), (_xm, 1, 1), (_os, 1, 2, 0),
        (_wfw, 0, 3, 1), (_os, 1, 3, 1), (_os, 1, 3, 0), (_of, 1, 0, 1), (_wfw, 1, 2, 1),
        (_xd, 1), (_xm, 0, 0), (_wzo, 1), (_wfw, 1, 0, 1), (_o1, 0, 0), (_wfw, 1, 0, 0),
        (_wl, 0), (_xt, 0, 0), (_of, 1, 2, 1), (_xm, 0, 1), (_wfw, 1, 1, 0), (_xt, 0, 1),
        (_mk, 1), (_xd, 0), (_wfw, 1, 1, 1), (_mk, 0), (_kvf, 2, 1), (_kvf, 2, 0),
        (_wfw, 1, 3, 1), (_of, 1, 1, 1), (_os, 0, 0, 1), (_wfw, 1, 3, 0), (_xt, 1, 0),
        (_xt, 1, 1), (_o3, 0), (_kvf, 3, 0), (_os, 0, 3, 0), (_kvf, 3, 1), (_xd, 2), (_mk, 2),
        (_os, 0, 0, 0), (_os, 0, 1, 0), (_kvf, 0, 0), (_os, 0, 1, 1), (_of, 1, 3, 1),
        (_kvf, 0, 1), (_os, 0, 3, 1), (_kvf, 1, 0), (_kvf, 1, 1), (_wl, 1), (_mq, 0),
        (_kvf, 4, 1), (_kvf, 4, 0), (_mq, 1), (_mq, 2), (_aw,), (_au, 0), (_au, 1), (_au, 2),
        (_os, 0, 2, 1), (_au, 3), (_of, 0, 1, 1), (_of, 1, 2, 0), (_ao, 0), (_os, 0, 2, 0),
        (_ao, 1), (_of, 0, 0, 1), (_of, 0, 3, 0), (_os, 1, 0, 0), (_of, 0, 3, 1), (_ao, 2),
        (_ao, 3), (_sw,), (_pj, 1), (_pj, 0), (_pj, 5), (_r1, 1), (_of, 0, 2, 1), (_pj, 3),
        (_r1, 0), (_of, 1, 0, 0), (_r1, 5), (_of, 0, 1, 0), (_of, 1, 1, 0), (_of, 0, 0, 0),
        (_of, 0, 2, 0), (_of, 1, 3, 0), (_r1, 3), (_r2, 1, 0), (_r2, 1, 1), (_r2, 0, 0),
        (_pj, 4), (_r2, 5, 1), (_pj, 2), (_r1, 4), (_r2, 3, 0), (_r2, 3, 1), (_r1, 2),
        (_pj, 6), (_r2, 4, 0), (_r2, 0, 1), (_r3, 1), (_r1, 6), (_r2, 4, 1), (_r2, 5, 0),
        (_pj, 7), (_r1, 7), (_r2, 2, 1), (_r3, 0), (_r3, 3), (_r2, 6, 0), (_r2, 2, 0),
        (_r2, 6, 1), (_r2, 7, 1), (_r2, 7, 0), (_r3, 2), (_r3, 6), (_r3, 5), (_r3, 4),
        (_r3, 7),
    ):
        fn(*nums)

    for i in range(16):
        zi, xi = i // 4, i % 4
        full[:, i * BLK:i * BLK + ON[0]] = sa[zi, :, xi * ON[0]:(xi + 1) * ON[0]]
        full[:, i * BLK + ON[0]:(i + 1) * BLK] = sb[xi, :, zi * ON[1]:(zi + 1) * ON[1]]

    def final(i, carry):
        rows = pl.ds(pl.multiple_of(i * 16, 16), 16)
        v = full[rows, :]
        r = lax.rsqrt(jnp.mean(v * v, axis=-1, keepdims=True) + EPSILON)
        out_v[rows, :] = (hid[rows, :].astype(F32) + v * r * post[...]).astype(BF)
        return carry

    lax.fori_loop(0, SUB // 16, final, 0)

    for p in range(2):
        remote(ws[p], ws[p], wsend.at[p], wrecv.at[p, 0], to_pt).wait_send()
    for col in range(2):
        ref = (oa, ob)[col].at[pl.ds(0, 15 * ON[col]), :]
        remote(ref, ref, osend.at[col], orecv.at[col, 0], to_pt).wait_send()
    ref = xs.at[pl.ds(0, 15 * SUB), :]
    remote(ref, ref, xsend, xrecv.at[0], to_pt).wait_send()
    for m in range(5):
        for i in range(2):

            @pl.when(c < 14)
            def _():
                kcopy(m, i).wait_send()

            @pl.when((cq, cn)[i] < 14)
            def _():
                kfinal(m, i, 1, to_xq).wait_send()

    for i in range(4):
        swap(i, False).wait_send()
    for q in range(8):
        r0copy(q).wait_send()
        for half in range(2):
            r1copy(q, half).wait_send()
            r2copy(q, half).wait_send()


def local(
    hidden_in, stretch_start, pre_gain, q_weight, k_weight, v_weight, o_weight, q_gain, k_gain,
    prior_keys, prior_values, post_gain,
):
    frequency = 10000.0 ** (-jnp.arange(HD // 2, dtype=F32) / (HD // 2))
    freq2 = jnp.concatenate([frequency, frequency]).reshape(1, HD)
    hbm = pl.BlockSpec(memory_space=pl.ANY)
    vm = pl.BlockSpec(memory_space=pltpu.VMEM)
    sm = pl.BlockSpec(memory_space=pltpu.SMEM)
    dma = pltpu.SemaphoreType.DMA
    return pl.pallas_call(
        body,
        out_shape=jax.ShapeDtypeStruct((SUB, D), BF),
        in_specs=[hbm, sm, hbm, hbm, hbm, hbm, hbm, vm, vm, hbm, hbm, hbm, vm],
        out_specs=vm,
        scratch_shapes=[
            pltpu.VMEM((D, 256), BF), pltpu.VMEM((D, 256), BF),
            pltpu.VMEM((16 * ON[0], 512), BF), pltpu.VMEM((16 * ON[1], 512), BF),
            pltpu.VMEM((2, 2, BLK, 256), BF), pltpu.VMEM((2, 2, 176, 256), BF),
            pltpu.VMEM((PAIR, D), BF),
            pltpu.VMEM((2, WINDOW + PAIR, HD), BF), pltpu.VMEM((2, 2, TOK, HD), BF),
            pltpu.VMEM((2, PAIR, HD), BF),
            pltpu.VMEM((2, TOK, 256), BF), pltpu.VMEM((TOK, 256), BF),
            pltpu.VMEM((TOK, 256), F32),
            pltpu.VMEM((SUB, D), BF), pltpu.VMEM((1, D), F32), pltpu.VMEM((1, D), F32),
            pltpu.VMEM((PAIR, HD), F32), pltpu.VMEM((PAIR, HD), F32),
            pltpu.VMEM((8, 4, 2, SUB, 768), BF),
            pltpu.VMEM((8, 4, SUB, 768), BF),
            pltpu.VMEM((8, 2, SUB // 2, 768), BF),
            pltpu.VMEM((8, 2, SUB, 768), BF),
            pltpu.VMEM((8, 3, SUB, 768), BF),
            pltpu.VMEM((4, SUB, CWP[0]), F32), pltpu.VMEM((4, SUB, CWP[1]), F32),
            pltpu.VMEM((SUB, D), F32),
            dma((16,)), dma((2,)), dma((2, 22)), dma((2,)), dma((2, 20)), dma, dma((26,)),
            dma((2, 5)), dma((2, 5)), dma((2, 5)), dma((2, 5)), dma((4,)), dma((4,)),
            dma((8, 5)), dma((8, 5)),
        ],
        compiler_params=pltpu.CompilerParams(
            collective_id=0, has_side_effects=True, vmem_limit_bytes=64 * 1024 * 1024 - 128 * 1024
        ),
        name="layer",
    )(
        hidden_in, stretch_start, pre_gain, q_weight, k_weight, v_weight,
        o_weight.T, q_gain.reshape(1, HD), k_gain.reshape(1, HD), prior_keys, prior_values,
        post_gain, freq2,
    )


def solution(mesh):
    return jax.shard_map(
        local,
        mesh=mesh,
        in_specs=(
            P(("ctx", "tp"), None), P(), P(), P("ctx", "tp"), P("ctx", "tp"), P("ctx", "tp"),
            P("tp", "ctx"), P(), P(), P(None, "tp"), P(None, "tp"), P(),
        ),
        out_specs=P(("ctx", "tp"), None),
        check_vma=False,
    )
```
